8 devices in a mesh: dp: 2 (over z, y), tp: 4 (over x, core).
Axes of the slice: x: 2, y: 2, z: 1, core: 2. Of those that a mesh axis runs over, the one named last changes fastest.
Arguments:
- node_lat: bfloat16 [2, 2562, 512], P('dp', None, 'tp')
- edge_lat: bfloat16 [2, 20460, 512], P('dp', None, 'tp')
- senders: int32 [20460], replicated
- receivers: int32 [20460], replicated
- grad_node: bfloat16 [2, 2562, 512], P('dp', None, 'tp')
- grad_edge: bfloat16 [2, 20460, 512], P('dp', None, 'tp')
- edge_w1: bfloat16 [2, 3, 512, 512], P(None, None, 'tp')
- edge_b1: float32 [2, 512], replicated
- edge_w2: bfloat16 [2, 512, 512], P(None, None, 'tp')
- edge_vec: float32 [2, 3, 512], P(None, None, 'tp')
- node_w1: bfloat16 [2, 2, 512, 512], P(None, None, 'tp')
- node_b1: float32 [2, 512], replicated
- node_w2: bfloat16 [2, 512, 512], P(None, None, 'tp')
- node_vec: float32 [2, 3, 512], P(None, None, 'tp')
Outputs:
- output 1: bfloat16 [2, 2562, 512], P('dp', None, 'tp')
- output 2: bfloat16 [2, 20460, 512], P('dp', None, 'tp')
- output 3: bfloat16 [2, 2562, 512], P('dp', None, 'tp')
- output 4: bfloat16 [2, 20460, 512], P('dp', None, 'tp')
- output 5: float32 [2, 3, 512, 512], P(None, None, 'tp')
- output 6: float32 [2, 512], replicated
- output 7: float32 [2, 512, 512], P(None, None, 'tp')
- output 8: float32 [2, 3, 512], P(None, None, 'tp')
- output 9: float32 [2, 2, 512, 512], P(None, None, 'tp')
- output 10: float32 [2, 512], replicated
- output 11: float32 [2, 512, 512], P(None, None, 'tp')
- output 12: float32 [2, 3, 512], P(None, None, 'tp')
All inputs are finite; a program needn't handle non-finite values.
Results may differ from the reference program's by a relative error of at most 0.02.
Values sent between devices are 32-bit elements.
A program may use at most 1 GiB of HBM per device.

```python
import jax
import jax.numpy as jnp
from jax import lax

D = 512
NODES = 2562
EDGES = 20460
BATCH = 2
LAYERS = 2
LN_EPS = 1e-5


def normal_draw(base_key, arr_shape):
    return jax.random.normal(base_key, arr_shape, jnp.float32)


def vec_draw(base_key):
    noise_val = normal_draw(base_key, (LAYERS, 3, D))
    scales = jnp.array([0.5, 0.3, 0.3], jnp.float32)[None, :, None]
    shifts = jnp.array([0.0, 1.0, 0.0], jnp.float32)[None, :, None]
    return noise_val * scales + shifts


def index_draw(base_key):
    idx_keys = jax.random.split(base_key, 4)
    extra_edges = EDGES - NODES
    senders = jnp.concatenate([
        jax.random.randint(idx_keys[0], (extra_edges,), 0, NODES, dtype=jnp.int32),
        jax.random.permutation(idx_keys[1], NODES).astype(jnp.int32)])
    receivers = jnp.concatenate([
        jax.random.permutation(idx_keys[2], NODES).astype(jnp.int32),
        jax.random.randint(idx_keys[3], (extra_edges,), 0, NODES, dtype=jnp.int32)])
    return senders, receivers


def setup_inputs(seed: int = 0) -> dict:
    sub_keys = jax.random.split(jax.random.key(seed), 13)
    senders, receivers = index_draw(sub_keys[12])
    node_shape = (BATCH, NODES, D)
    edge_shape = (BATCH, EDGES, D)
    return {
        'node_lat': normal_draw(sub_keys[0], node_shape).astype(jnp.bfloat16),
        'edge_lat': normal_draw(sub_keys[1], edge_shape).astype(jnp.bfloat16),
        'senders': senders,
        'receivers': receivers,
        'grad_node': normal_draw(sub_keys[2], node_shape).astype(jnp.bfloat16),
        'grad_edge': normal_draw(sub_keys[3], edge_shape).astype(jnp.bfloat16),
        'edge_w1': (normal_draw(sub_keys[4], (LAYERS, 3, D, D)) * (3 * D) ** -0.5).astype(jnp.bfloat16),
        'edge_b1': 0.5 * normal_draw(sub_keys[5], (LAYERS, D)),
        'edge_w2': (normal_draw(sub_keys[6], (LAYERS, D, D)) * D ** -0.5).astype(jnp.bfloat16),
        'edge_vec': vec_draw(sub_keys[7]),
        'node_w1': (normal_draw(sub_keys[8], (LAYERS, 2, D, D)) * (2 * D) ** -0.5).astype(jnp.bfloat16),
        'node_b1': 0.5 * normal_draw(sub_keys[9], (LAYERS, D)),
        'node_w2': (normal_draw(sub_keys[10], (LAYERS, D, D)) * D ** -0.5).astype(jnp.bfloat16),
        'node_vec': vec_draw(sub_keys[11]),
    }


def mlp_norm(inputs, w_first, b_first, w_second, norm_vec):
    hidden = b_first
    for block_id in range(len(inputs)):
        hidden = hidden + jnp.dot(inputs[block_id], w_first[block_id].astype(jnp.bfloat16), preferred_element_type=jnp.float32)
    act_bf = jax.nn.silu(hidden).astype(jnp.bfloat16)
    out_f32 = jnp.dot(act_bf, w_second.astype(jnp.bfloat16), preferred_element_type=jnp.float32) + norm_vec[0]
    row_mean = jnp.mean(out_f32, axis=-1, keepdims=True)
    centered = out_f32 - row_mean
    row_var = jnp.mean(centered * centered, axis=-1, keepdims=True)
    return (centered * lax.rsqrt(row_var + LN_EPS) * norm_vec[1] + norm_vec[2]).astype(jnp.bfloat16)


def layer_step(node_lat, edge_lat, senders, receivers, layer_par):
    edge_w1, edge_b1, edge_w2, edge_vec, node_w1, node_b1, node_w2, node_vec = layer_par
    send_lat = jnp.take(node_lat, senders, axis=0)
    recv_lat = jnp.take(node_lat, receivers, axis=0)
    edge_msg = mlp_norm((edge_lat, send_lat, recv_lat), edge_w1, edge_b1, edge_w2, edge_vec)
    node_agg = jax.ops.segment_sum(edge_msg.astype(jnp.float32), receivers, num_segments=node_lat.shape[0]).astype(jnp.bfloat16)
    node_msg = mlp_norm((node_lat, node_agg), node_w1, node_b1, node_w2, node_vec)
    new_node = (node_lat.astype(jnp.float32) + node_msg.astype(jnp.float32)).astype(jnp.bfloat16)
    new_edge = (edge_lat.astype(jnp.float32) + edge_msg.astype(jnp.float32)).astype(jnp.bfloat16)
    return new_node, new_edge


def sample_forward(node_lat, edge_lat, senders, receivers, params):
    def layer_body(carry_lat, layer_par):
        return layer_step(carry_lat[0], carry_lat[1], senders, receivers, layer_par), None
    final_lat, unused_out = lax.scan(layer_body, (node_lat, edge_lat), params)
    return final_lat


def reference(node_lat, edge_lat, senders, receivers, grad_node, grad_edge, edge_w1, edge_b1, edge_w2, edge_vec, node_w1, node_b1, node_w2, node_vec):
    params = (edge_w1.astype(jnp.float32), edge_b1, edge_w2.astype(jnp.float32), edge_vec,
              node_w1.astype(jnp.float32), node_b1, node_w2.astype(jnp.float32), node_vec)

    def forward_fn(node_one, edge_one, par_f32):
        return sample_forward(node_one, edge_one, senders, receivers, par_f32)

    def per_sample(grad_acc, sample):
        node_one, edge_one, gnode_one, gedge_one = sample
        fwd_outs, pullback = jax.vjp(forward_fn, node_one, edge_one, params)
        d_node, d_edge, d_params = pullback((gnode_one, gedge_one))
        grad_acc = tuple(acc_part + new_part for acc_part, new_part in zip(grad_acc, d_params))
        return grad_acc, (fwd_outs[0], fwd_outs[1], d_node, d_edge)

    zero_acc = tuple(jnp.zeros(par_arr.shape, jnp.float32) for par_arr in params)
    grad_acc, per_out = lax.scan(per_sample, zero_acc, (node_lat, edge_lat, grad_node, grad_edge))
    return (per_out[0], per_out[1], per_out[2], per_out[3],
            grad_acc[0], grad_acc[1], grad_acc[2], grad_acc[3],
            grad_acc[4], grad_acc[5], grad_acc[6], grad_acc[7])
```

```python
import functools

import jax
import jax.numpy as jnp
from jax import lax
from jax.experimental import pallas as pl
from jax.experimental.pallas import tpu as pltpu
from jax.sharding import PartitionSpec as P

LN_EPS = 1e-5
F32 = jnp.float32
BF16 = jnp.bfloat16
LANES = 128
EDGE_BLK = 256
NODE_BLK = 368
GATHER_UNROLL = 16
ALL = Ellipsis
FULL = (slice(None), slice(None))
VMEM_BYTES = 64 * 2**20 - 2**16


WORK = 4 * 10**9


def slot_views(pair_a, pair_b):
    return pair_a.at[0], pair_b.at[0], pair_a.at[1], pair_b.at[1]


def dot(lhs, rhs):
    return lax.dot_general(lhs, rhs, (((1,), (0,)), ((), ())), preferred_element_type=F32)


def dot_tb(lhs, rhs):
    return lax.dot_general(lhs, rhs, (((1,), (1,)), ((), ())), preferred_element_type=F32)


def dot_ta(lhs, rhs):
    return lax.dot_general(lhs, rhs, (((0,), (0,)), ((), ())), preferred_element_type=F32)


def col(val, slot):
    return val[:, slot * LANES:(slot + 1) * LANES]


def gather_rows(tables, index_refs, base, out_ref, num_rows):
    def step(it, carry):
        for sub in range(GATHER_UNROLL):
            row = it * GATHER_UNROLL + sub
            acc = None
            for table, index_ref in zip(tables, index_refs):
                val = table[pl.ds(pl.multiple_of(index_ref[base + row], 4), 4), :]
                acc = val if acc is None else acc + val
            out_ref[pl.ds(pl.multiple_of(row * 4, 4), 4), :] = acc
        return carry
    lax.fori_loop(0, num_rows // GATHER_UNROLL, step, 0)


def scatter_rows(accs, index_refs, base, src_ref, num_rows, copies, stride):
    def step(it, carry):
        pending = []
        for sub in range(copies):
            row = it * copies + sub
            val = src_ref[pl.ds(pl.multiple_of(row * 4, 4), 4), :]
            for acc, index_ref in zip(accs, index_refs):
                at = pl.multiple_of(index_ref[base + row] + sub * stride, 4)
                pending.append((acc, at, acc[pl.ds(at, 4), :] + val))
        for acc, at, val in pending:
            acc[pl.ds(at, 4), :] = val
        return carry
    lax.fori_loop(0, num_rows // copies, step, 0)


def zero_rows(ref, rows, step_rows):
    def step(it, carry):
        ref[pl.ds(pl.multiple_of(it * step_rows, 8), step_rows), :] = jnp.zeros((step_rows, LANES), F32)
        return carry
    lax.fori_loop(0, rows // step_rows, step, 0)


def row_mean(val):
    return jnp.sum(val, axis=-1, keepdims=True) * (1.0 / val.shape[-1])


def mlp_tail(hidden, w2t, vec_ref):
    act = (hidden * jax.nn.sigmoid(hidden)).astype(BF16)
    out = dot_tb(act, w2t) + vec_ref[0:1, :]
    centered = out - row_mean(out)
    inv_std = lax.rsqrt(row_mean(centered * centered) + LN_EPS)
    normed = centered * inv_std
    message = (normed * vec_ref[1:2, :] + vec_ref[2:3, :]).astype(BF16)
    return act, normed, inv_std, message


def mlp_back(d_message, hidden, normed, inv_std, w2t, vec_ref):
    d_normed = d_message * vec_ref[1:2, :]
    d_out = inv_std * (d_normed - row_mean(d_normed) - normed * row_mean(d_normed * normed))
    d_out_bf = d_out.astype(BF16)
    sig = jax.nn.sigmoid(hidden)
    act = (hidden * sig).astype(BF16)
    d_act = dot(d_out_bf, w2t)
    d_hidden = d_act * (sig * (1.0 + hidden * (1.0 - sig)))
    sums = [jnp.sum(x, axis=0, keepdims=True) for x in (d_out, d_message * normed, d_message, d_hidden)]
    return d_out_bf, act, d_hidden, sums


def add_to(ref, idx, val, first):
    @pl.when(first)
    def _():
        ref[idx] = val

    @pl.when(jnp.logical_not(first))
    def _():
        ref[idx] += val


def call(body, grid, in_specs, out_specs, out_shape, scratch, name, prefetch=0, work=1):
    return pl.pallas_call(
        body,
        out_shape=out_shape,
        grid_spec=pltpu.PrefetchScalarGridSpec(
            num_scalar_prefetch=prefetch, grid=grid, in_specs=in_specs, out_specs=out_specs, scratch_shapes=scratch),
        compiler_params=pltpu.CompilerParams(vmem_limit_bytes=VMEM_BYTES, dimension_semantics=("arbitrary",) * len(grid)),
        cost_estimate=pl.CostEstimate(flops=work * WORK, bytes_accessed=work * WORK // 1000, transcendentals=0),
        name=name)


def rows_spec(blk, width):
    return pl.BlockSpec((blk, width), lambda i, *_: (i, 0))


def whole_spec(shape):
    zeros = (0,) * len(shape)
    return pl.BlockSpec(shape, lambda i, *_: zeros, pipeline_mode=pl.Buffered(1))


def pair_spec(blk):
    return pl.BlockSpec((2, blk, LANES), lambda i, *_: (0, i, 0))


def sds(shape, dtype):
    return jax.ShapeDtypeStruct(shape, dtype)


def edge_fwd_body(n_in, last, pad_nodes, copies, snd_ref, rcv_ref, *refs):
    x_refs = refs[:n_in]
    ps_ref, pr_ref, w1_ref, w2t_ref, vec_ref, hid_ref, nrm_ref, inv_ref = refs[n_in:n_in + 8]
    n_out = 4 if last else 1
    new_refs = refs[n_in + 8:n_in + 8 + n_out]
    sa_ref, sb_ref, gat_ref, msg_ref, acc_ref = refs[n_in + 8 + n_out:]
    step = pl.program_id(0)
    base = step * EDGE_BLK
    stride = 4 * pad_nodes

    @pl.when(step == 0)
    def _():
        zero_rows(acc_ref, stride * copies, stride // 4)

    gather_rows((ps_ref, pr_ref), (snd_ref, rcv_ref), base, gat_ref, EDGE_BLK)
    x_in = jnp.concatenate([ref[ALL].astype(BF16) for ref in x_refs], axis=-1)
    part = dot(x_in, w1_ref[ALL])
    hidden = jnp.concatenate(
        [col(part, slot) + gat_ref[pl.ds(slot, EDGE_BLK, stride=4), :] for slot in range(4)], axis=-1)
    hid_ref[ALL] = hidden
    _, normed, inv_std, message = mlp_tail(hidden, w2t_ref[ALL], vec_ref)
    nrm_ref[ALL] = normed
    inv_ref[ALL] = jnp.broadcast_to(inv_std, (EDGE_BLK, LANES))
    msg = message.astype(F32)
    new = (x_in.astype(F32) + msg).astype(BF16)
    if last:
        for slot in range(4):
            new_refs[slot][ALL] = col(new, slot).astype(new_refs[slot].dtype)
    else:
        new_refs[0][ALL] = new
    for slot in range(4):
        msg_ref[pl.ds(slot, EDGE_BLK, stride=4), :] = col(msg, slot)
    scatter_rows((acc_ref,), (rcv_ref,), base, msg_ref, EDGE_BLK, copies, stride)

    @pl.when(step == pl.num_programs(0) - 1)
    def _():
        def fin(it, carry):
            for slot, out in enumerate(slot_views(sa_ref, sb_ref)):
                total = acc_ref[pl.ds(it * (4 * NODE_BLK) + slot, NODE_BLK, stride=4), :]
                for cp in range(1, copies):
                    total = total + acc_ref[pl.ds(it * (4 * NODE_BLK) + slot + cp * stride, NODE_BLK, stride=4), :]
                out[pl.ds(pl.multiple_of(it * NODE_BLK, 8), NODE_BLK), :] = total
            return carry
        lax.fori_loop(0, pad_nodes // NODE_BLK, fin, 0)


def edge_forward(snd, rcv, xs, ps, pr, w1, w2t, vec, last, pad_nodes):
    rows, width = snd.shape[0], w1.shape[0]
    copies = 4
    n_in = len(xs)
    slot_shapes = [sds((rows, LANES), BF16)] + [sds((rows, LANES), F32)] * 3
    new_shapes = slot_shapes if last else [sds((rows, width), BF16)]
    outs = [sds((rows, width), F32), sds((rows, width), F32), sds((rows, LANES), F32)] + new_shapes
    outs += [sds((2, pad_nodes, LANES), F32)] * 2
    in_specs = [rows_spec(EDGE_BLK, x.shape[1]) for x in xs]
    in_specs += [whole_spec(a.shape) for a in (ps, pr, w1, w2t, vec)]
    out_specs = [rows_spec(EDGE_BLK, o.shape[1]) for o in outs[:-2]] + [whole_spec(o.shape) for o in outs[-2:]]
    scratch = [pltpu.VMEM((4 * EDGE_BLK, LANES), F32), pltpu.VMEM((4 * EDGE_BLK, LANES), F32),
               pltpu.VMEM((copies * 4 * pad_nodes, LANES), F32)]
    return call(functools.partial(edge_fwd_body, n_in, last, pad_nodes, copies), (rows // EDGE_BLK,), in_specs, out_specs,
                outs, scratch, "edge_fwd", prefetch=2, work=12)(snd, rcv, *xs, ps, pr, w1, w2t, vec)


def edge_bwd_body(n_in, last, pad_nodes, copies, snd_ref, rcv_ref, *refs):
    n_g = 4 if last else 1
    g_refs = refs[:n_g]
    x_refs = refs[n_g:n_g + n_in]
    hid_ref, nrm_ref, inv_ref, ds_ref, w1_ref, w2t_ref, vec_ref = refs[n_g + n_in:n_g + n_in + 7]
    rest = refs[n_g + n_in + 7:]
    n_out = 1 if last else 4
    d_refs = rest[:n_out]
    dw1_ref, dw2t_ref, small_ref, ts_ref, tr_ref, gat_ref, dh_ref, accs_ref, accr_ref = rest[n_out:]
    step = pl.program_id(0)
    base = step * EDGE_BLK
    stride = 4 * pad_nodes
    first = step == 0

    @pl.when(first)
    def _():
        zero_rows(accs_ref, stride * copies, stride // 4)
        zero_rows(accr_ref, stride * copies, stride // 4)

    gather_rows((ds_ref,), (rcv_ref,), base, gat_ref, EDGE_BLK)
    d_edge = jnp.concatenate([ref[ALL].astype(F32) for ref in g_refs], axis=-1)
    d_message = jnp.concatenate(
        [col(d_edge, slot) + gat_ref[pl.ds(slot, EDGE_BLK, stride=4), :] for slot in range(4)], axis=-1)
    d_out_bf, act, d_hidden, sums = mlp_back(
        d_message, hid_ref[ALL], nrm_ref[ALL], inv_ref[:, 0:1], w2t_ref[ALL], vec_ref)
    d_hidden_bf = d_hidden.astype(BF16)
    x_in = jnp.concatenate([ref[ALL].astype(BF16) for ref in x_refs], axis=-1)
    add_to(dw2t_ref, FULL, dot_ta(d_out_bf, act), first)
    add_to(dw1_ref, FULL, dot_ta(x_in, d_hidden_bf), first)
    add_to(small_ref, (slice(0, 4), slice(None)), jnp.concatenate(sums, axis=0), first)
    d_x = (d_edge + dot_tb(d_hidden_bf, w1_ref[ALL])).astype(BF16)
    if last:
        d_refs[0][ALL] = d_x
    else:
        for slot in range(4):
            d_refs[slot][ALL] = col(d_x, slot).astype(d_refs[slot].dtype)
    for slot in range(4):
        dh_ref[pl.ds(slot, EDGE_BLK, stride=4), :] = col(d_hidden, slot)
    scatter_rows((accs_ref, accr_ref), (snd_ref, rcv_ref), base, dh_ref, EDGE_BLK, copies, stride)

    @pl.when(step == pl.num_programs(0) - 1)
    def _():
        small_ref[4:8, :] = jnp.zeros((4, small_ref.shape[1]), F32)

        def fin(it, carry):
            for acc_ref, out_ref in ((accs_ref, ts_ref), (accr_ref, tr_ref)):
                for slot in range(4):
                    total = acc_ref[pl.ds(it * (4 * NODE_BLK) + slot, NODE_BLK, stride=4), :]
                    for cp in range(1, copies):
                        total = total + acc_ref[pl.ds(it * (4 * NODE_BLK) + slot + cp * stride, NODE_BLK, stride=4), :]
                    out_ref[pl.ds(pl.multiple_of(it * NODE_BLK, 16), NODE_BLK),
                            slot * LANES:(slot + 1) * LANES] = total.astype(BF16)
            return carry
        lax.fori_loop(0, pad_nodes // NODE_BLK, fin, 0)


def edge_backward(snd, rcv, gs, xs, saved, ds, w1, w2t, vec, last, pad_nodes):
    rows, width = snd.shape[0], w1.shape[0]
    copies = 2
    hid, nrm, inv = saved
    slot_shapes = [sds((rows, LANES), BF16)] + [sds((rows, LANES), F32)] * 3
    d_shapes = [sds((rows, width), BF16)] if last else slot_shapes
    tail = [sds((width, width), F32), sds((width, width), F32), sds((8, width), F32),
            sds((pad_nodes, width), BF16), sds((pad_nodes, width), BF16)]
    ins = list(gs) + list(xs) + [hid, nrm, inv]
    in_specs = [rows_spec(EDGE_BLK, x.shape[1]) for x in ins] + [whole_spec(a.shape) for a in (ds, w1, w2t, vec)]
    out_specs = [rows_spec(EDGE_BLK, o.shape[1]) for o in d_shapes] + [whole_spec(o.shape) for o in tail]
    scratch = [pltpu.VMEM((4 * EDGE_BLK, LANES), F32), pltpu.VMEM((4 * EDGE_BLK, LANES), F32),
               pltpu.VMEM((copies * 4 * pad_nodes, LANES), F32), pltpu.VMEM((copies * 4 * pad_nodes, LANES), F32)]
    return call(functools.partial(edge_bwd_body, len(xs), last, pad_nodes, copies), (rows // EDGE_BLK,), in_specs, out_specs,
                d_shapes + tail, scratch, "edge_bwd", prefetch=2, work=20)(snd, rcv, *ins, ds, w1, w2t, vec)


def proj_bwd_body(ts_ref, tr_ref, v_ref, w1s_ref, w1r_ref, dw1e_ref, dw2t_ref, small_ref, node_b1_ref,
                  da_ref, db_ref, ga_ref, gb_ref, acc_s, acc_r):
    step = pl.program_id(0)
    first = step == 0
    d_v = dot_tb(ts_ref[ALL], w1s_ref[ALL]) + dot_tb(tr_ref[ALL], w1r_ref[ALL])
    for slot, out in enumerate(slot_views(da_ref, db_ref)):
        out[ALL] = col(d_v, slot)
    add_to(acc_s, FULL, dot_ta(v_ref[ALL], ts_ref[ALL]), first)
    add_to(acc_r, FULL, dot_ta(v_ref[ALL], tr_ref[ALL]), first)

    @pl.when(step == pl.num_programs(0) - 1)
    def _():
        for slot, out in enumerate(slot_views(ga_ref, gb_ref)):
            rows = slice(slot * LANES, (slot + 1) * LANES)
            for part, src in enumerate((dw1e_ref, acc_s, acc_r, dw2t_ref)):
                out[part * LANES:(part + 1) * LANES, :] = src[rows, :]
            vec_row = jnp.concatenate(
                [small_ref[k:k + 1, rows] for k in range(3)] + [jnp.zeros((1, LANES), F32)], axis=-1)
            out[512:520, :] = jnp.concatenate(
                [vec_row, small_ref[3:4, :], node_b1_ref[0:1, :], jnp.zeros((5, vec_row.shape[1]), F32)], axis=0)


def proj_backward(ts, tr, v_full, w1s, w1r, dw1e, dw2t, small, node_b1):
    nodes, width = v_full.shape
    ins = [ts, tr, v_full, w1s, w1r, dw1e, dw2t, small, node_b1]
    outs = [sds((2, nodes, LANES), F32)] * 2 + [sds((2, width + 8, width), F32)] * 2
    in_specs = [rows_spec(NODE_BLK, width)] * 3 + [whole_spec(a.shape) for a in ins[3:]]
    out_specs = [pair_spec(NODE_BLK)] * 2 + [whole_spec(outs[2].shape)] * 2
    scratch = [pltpu.VMEM((width, width), F32)] * 2
    return call(proj_bwd_body, (nodes // NODE_BLK,), in_specs, out_specs, outs, scratch, "proj_bwd")(*ins)


def write_table(ref, val):
    for slot in range(4):
        ref[pl.ds(slot, NODE_BLK, stride=4), :] = col(val, slot)


def node_proj_body(v0_ref, v1_ref, v2_ref, v3_ref, w1s_ref, w1r_ref, b1_ref, v_ref, ps_ref, pr_ref):
    v_in = jnp.concatenate([ref[ALL].astype(BF16) for ref in (v0_ref, v1_ref, v2_ref, v3_ref)], axis=-1)
    v_ref[ALL] = v_in
    write_table(ps_ref, dot(v_in, w1s_ref[ALL]) + b1_ref[0:1, :])
    write_table(pr_ref, dot(v_in, w1r_ref[ALL]))


def node_project(vs, w1s, w1r, b1):
    nodes, width = vs[0].shape[0], w1s.shape[0]
    in_specs = [rows_spec(NODE_BLK, LANES)] * 4 + [whole_spec(a.shape) for a in (w1s, w1r, b1)]
    outs = [sds((nodes, width), BF16), sds((4 * nodes, LANES), F32), sds((4 * nodes, LANES), F32)]
    out_specs = [rows_spec(NODE_BLK, width)] + [rows_spec(4 * NODE_BLK, LANES)] * 2
    return call(node_proj_body, (nodes // NODE_BLK,), in_specs, out_specs, outs, [], "node_proj")(
        *vs, w1s, w1r, b1)


def read_pairs(a_ref, b_ref):
    return jnp.concatenate([a_ref[0], b_ref[0], a_ref[1], b_ref[1]], axis=-1)


def node_fwd_body(v_ref, sa_ref, sb_ref, w1_ref, w2t_ref, vec_ref, b1_ref, w1s_ref, w1r_ref, eb1_ref,
                  new_ref, s_ref, hid_ref, nrm_ref, inv_ref, ps_ref, pr_ref):
    v_in = v_ref[ALL]
    s_in = read_pairs(sa_ref, sb_ref).astype(BF16)
    s_ref[ALL] = s_in
    hidden = dot(v_in, w1_ref[0]) + dot(s_in, w1_ref[1]) + b1_ref[0:1, :]
    hid_ref[ALL] = hidden
    _, normed, inv_std, message = mlp_tail(hidden, w2t_ref[ALL], vec_ref)
    nrm_ref[ALL] = normed
    inv_ref[ALL] = jnp.broadcast_to(inv_std, (NODE_BLK, LANES))
    new = (v_in.astype(F32) + message.astype(F32)).astype(BF16)
    new_ref[ALL] = new
    write_table(ps_ref, dot(new, w1s_ref[ALL]) + eb1_ref[0:1, :])
    write_table(pr_ref, dot(new, w1r_ref[ALL]))


def node_forward(v_in, sa, sb, w1, w2t, vec, b1, w1s, w1r, eb1):
    nodes, width = v_in.shape
    in_specs = [rows_spec(NODE_BLK, width), pair_spec(NODE_BLK), pair_spec(NODE_BLK)]
    in_specs += [whole_spec(a.shape) for a in (w1, w2t, vec, b1, w1s, w1r, eb1)]
    outs = [sds((nodes, width), BF16), sds((nodes, width), BF16), sds((nodes, width), F32), sds((nodes, width), F32),
            sds((nodes, LANES), F32), sds((4 * nodes, LANES), F32), sds((4 * nodes, LANES), F32)]
    out_specs = [rows_spec(NODE_BLK, o.shape[1]) for o in outs[:5]] + [rows_spec(4 * NODE_BLK, LANES)] * 2
    return call(node_fwd_body, (nodes // NODE_BLK,), in_specs, out_specs, outs, [], "node_fwd")(
        v_in, sa, sb, w1, w2t, vec, b1, w1s, w1r, eb1)


def node_grads(first, d_message, v_in, s_in, hidden, normed, inv_std, w1_ref, w2t_ref, vec_ref, ds_ref, gn_ref, db1_ref):
    d_out_bf, act, d_hidden, sums = mlp_back(d_message, hidden, normed, inv_std, w2t_ref[ALL], vec_ref)
    d_hidden_bf = d_hidden.astype(BF16)
    write_table(ds_ref, dot_tb(d_hidden_bf, w1_ref[1]))
    whole = slice(None)
    add_to(gn_ref, (slice(0, LANES), whole), dot_ta(col(v_in, 0), d_hidden_bf), first)
    add_to(gn_ref, (slice(LANES, 2 * LANES), whole), dot_ta(col(s_in, 0), d_hidden_bf), first)
    add_to(gn_ref, (slice(2 * LANES, 3 * LANES), whole), dot_ta(col(d_out_bf, 0), act), first)
    vec_row = jnp.concatenate([col(x, 0) for x in sums[:3]] + [jnp.zeros((1, LANES), F32)], axis=-1)
    add_to(gn_ref, (slice(3 * LANES, 3 * LANES + 8), whole),
           jnp.concatenate([vec_row, jnp.zeros((7, vec_row.shape[1]), F32)], axis=0), first)
    add_to(db1_ref, (whole, whole), jnp.broadcast_to(sums[3], db1_ref.shape), first)
    return dot_tb(d_hidden_bf, w1_ref[0])


def node_top_body(v_ref, sa_ref, sb_ref, g0_ref, g1_ref, g2_ref, g3_ref, w1_ref, w2t_ref, vec_ref, b1_ref,
                  new_ref, ds_ref, dv_ref, gn_ref, db1_ref):
    first = pl.program_id(0) == 0
    v_in = v_ref[ALL]
    s_in = read_pairs(sa_ref, sb_ref).astype(BF16)
    hidden = dot(v_in, w1_ref[0]) + dot(s_in, w1_ref[1]) + b1_ref[0:1, :]
    _, normed, inv_std, message = mlp_tail(hidden, w2t_ref[ALL], vec_ref)
    new_ref[ALL] = (col(v_in, 0).astype(F32) + col(message, 0).astype(F32)).astype(BF16)
    d_new = jnp.concatenate([ref[ALL].astype(F32) for ref in (g0_ref, g1_ref, g2_ref, g3_ref)], axis=-1)
    dv_ref[ALL] = d_new + node_grads(
        first, d_new, v_in, s_in, hidden, normed, inv_std, w1_ref, w2t_ref, vec_ref, ds_ref, gn_ref, db1_ref)


def node_top(v_in, sa, sb, gs, w1, w2t, vec, b1):
    nodes, width = v_in.shape
    in_specs = [rows_spec(NODE_BLK, width), pair_spec(NODE_BLK), pair_spec(NODE_BLK)] + [rows_spec(NODE_BLK, LANES)] * 4
    in_specs += [whole_spec(a.shape) for a in (w1, w2t, vec, b1)]
    outs = [sds((nodes, LANES), BF16), sds((4 * nodes, LANES), F32), sds((nodes, width), F32),
            sds((3 * LANES + 8, width), F32), sds((8, width), F32)]
    out_specs = [rows_spec(NODE_BLK, LANES), rows_spec(4 * NODE_BLK, LANES), rows_spec(NODE_BLK, width),
                 whole_spec(outs[3].shape), whole_spec(outs[4].shape)]
    return call(node_top_body, (nodes // NODE_BLK,), in_specs, out_specs, outs, [], "node_top")(
        v_in, sa, sb, *gs, w1, w2t, vec, b1)


def node_bwd_body(dv_ref, ta_ref, tb_ref, v_ref, s_ref, hid_ref, nrm_ref, inv_ref, w1_ref, w2t_ref, vec_ref,
                  ds_ref, dvo_ref, gn_ref, db1_ref):
    first = pl.program_id(0) == 0
    d_new = (dv_ref[ALL] + read_pairs(ta_ref, tb_ref)).astype(BF16).astype(F32)
    d_v = node_grads(first, d_new, v_ref[ALL], s_ref[ALL], hid_ref[ALL], nrm_ref[ALL], inv_ref[:, 0:1],
                     w1_ref, w2t_ref, vec_ref, ds_ref, gn_ref, db1_ref)
    dvo_ref[ALL] = col(d_new, 0) + col(d_v, 0)


def node_backward(dv, ta, tb, v_in, s_in, saved, w1, w2t, vec):
    nodes, width = v_in.shape
    ins = [dv, ta, tb, v_in, s_in, *saved]
    in_specs = [rows_spec(NODE_BLK, width), pair_spec(NODE_BLK), pair_spec(NODE_BLK)]
    in_specs += [rows_spec(NODE_BLK, a.shape[1]) for a in ins[3:]] + [whole_spec(a.shape) for a in (w1, w2t, vec)]
    outs = [sds((4 * nodes, LANES), F32), sds((nodes, LANES), F32), sds((3 * LANES + 8, width), F32), sds((8, width), F32)]
    out_specs = [rows_spec(4 * NODE_BLK, LANES), rows_spec(NODE_BLK, LANES), whole_spec(outs[2].shape),
                 whole_spec(outs[3].shape)]
    return call(node_bwd_body, (nodes // NODE_BLK,), in_specs, out_specs, outs, [], "node_bwd")(
        *ins, w1, w2t, vec)


def to_slots_body(limit, me_ref, x_ref, *out_refs):
    part, slot = pl.program_id(0), pl.program_id(1)
    blk = x_ref.shape[0]
    at = ((me_ref[0] ^ slot) * pl.num_programs(0) + part) * blk
    row = lax.broadcasted_iota(jnp.int32, x_ref.shape, 0) + at
    val = jnp.where(row < limit, x_ref[ALL].astype(F32), 0.0)
    for k, out in enumerate(out_refs):
        @pl.when(slot == k)
        def _():
            out[ALL] = val.astype(out.dtype)


def to_slots(me, val, rows):
    limit, parts = val.shape[0], 2
    blk = rows // parts
    outs = [sds((rows, LANES), BF16)] + [sds((rows, LANES), F32)] * 3
    return call(functools.partial(to_slots_body, limit), (parts, 4),
                [pl.BlockSpec((blk, LANES), lambda r, d, me: ((me[0] ^ d) * parts + r, 0))],
                [pl.BlockSpec((blk, LANES), lambda r, d, me: (r, 0))] * 4, outs, [], "to_slots", prefetch=1)(me, val)


def from_slots_body(me_ref, *refs):
    out_ref = refs[-1]
    for k, ref in enumerate(refs[:-1]):
        @pl.when(pl.program_id(1) == k)
        def _():
            out_ref[ALL] = ref[ALL].astype(BF16)


def from_slots(me, slots, limit):
    rows, parts = slots[0].shape[0], 2
    blk = rows // parts
    return call(from_slots_body, (parts, 4), [pl.BlockSpec((blk, LANES), lambda r, d, me: (r, 0))] * 4,
                pl.BlockSpec((blk, LANES), lambda r, d, me: ((me[0] ^ d) * parts + r, 0)), sds((limit, LANES), BF16), [],
                "from_slots", prefetch=1)(me, *slots)


def unpack_body(starts, *refs):
    slots, outs = refs[:4], refs[4:]
    for at, out in zip(starts, outs):
        for k, ref in enumerate(slots):
            out[k * LANES:(k + 1) * LANES, :] = ref[at:at + LANES, :].astype(BF16)


def unpack_weights(slots, starts):
    width = slots[0].shape[1]
    outs = [sds((4 * LANES, width), BF16)] * len(starts)
    return call(functools.partial(unpack_body, starts), (1,), [whole_spec(s.shape) for s in slots],
                [whole_spec(o.shape) for o in outs], outs, [], "unpack")(*slots)


def solution(mesh):
    lat_spec = P('dp', None, 'tp')
    first_spec = P(None, None, 'tp', None)
    col_spec = P(None, None, 'tp')
    param_specs = (first_spec, P(), col_spec, col_spec, first_spec, P(), col_spec, col_spec)
    in_specs = (lat_spec, lat_spec, P(), P(), lat_spec, lat_spec) + param_specs
    out_specs = (lat_spec, lat_spec, lat_spec, lat_spec) + param_specs
    tp = mesh.shape['tp']

    def swap(val, mask):
        return lax.ppermute(val, 'tp', [(i, i ^ mask) for i in range(tp)])

    def swap_dp(val):
        return lax.ppermute(val, 'dp', [(0, 1), (1, 0)])

    def slots_of(val):
        far = swap(val, 2)
        return val, swap(val, 1), far, swap(far, 1)

    def local_step(node_lat, edge_lat, senders, receivers, grad_node, grad_edge,
                   edge_w1, edge_b1, edge_w2, edge_vec, node_w1, node_b1, node_w2, node_vec):
        me = lax.axis_index('tp')
        nodes, edges = node_lat.shape[1], edge_lat.shape[1]
        width = edge_w2.shape[1]
        rows = -(-edges // (tp * EDGE_BLK)) * EDGE_BLK
        pad_nodes = (nodes // NODE_BLK + 1) * NODE_BLK

        me_ref = me.astype(jnp.int32)[None]

        def to_rows(val):
            blocks = to_slots(me_ref, val, rows)
            return [blocks[0]] + [swap(blocks[d], d) for d in range(1, tp)]

        def to_columns(slots):
            return from_slots(me_ref, [slots[0]] + [swap(slots[d], d) for d in range(1, tp)], edges)[None]

        def my_index(ids):
            padded = jnp.pad(ids, (0, tp * rows - edges), constant_values=nodes)
            return lax.dynamic_slice(padded, (me * rows,), (rows,)) * 4

        snd, rcv = my_index(senders), my_index(receivers)

        def pack(l, w1, w2):
            return jnp.concatenate([w1[l].reshape(-1, width), w2[l].T], axis=0).astype(F32)

        vecs = jnp.concatenate([edge_vec.reshape(-1), node_vec.reshape(-1)]).reshape(-1, width)
        vecs = jnp.pad(vecs, ((0, 8 - vecs.shape[0]), (0, 0)))
        group_a = jnp.concatenate([pack(0, edge_w1, edge_w2), vecs], axis=0)
        group_b = jnp.concatenate([pack(0, node_w1, node_w2), pack(1, edge_w1, edge_w2), pack(1, node_w1, node_w2)], axis=0)
        v_pad = jnp.pad(node_lat[0], ((0, pad_nodes - nodes), (0, 0)))
        v_slots = slots_of(v_pad.astype(F32))
        slots_a = slots_of(group_a)
        x_slots = to_rows(edge_lat[0])
        slots_b = slots_of(group_b)
        g_slots = to_rows(grad_edge[0])
        gn_pad = jnp.pad(grad_node[0], ((0, pad_nodes - nodes), (0, 0)))
        gn_slots = slots_of(gn_pad.astype(F32))

        mats_a = unpack_weights(slots_a, (0, 128, 256, 384))
        mats_b = unpack_weights(slots_b, tuple(range(0, 1280, 128)))
        ew, nw = [mats_a, mats_b[3:7]], [mats_b[:3], mats_b[7:]]
        all_vec = jnp.stack([s[512:515].reshape(2, 2, 3, LANES) for s in slots_a], axis=3).reshape(2, 2, 3, width)
        all_vec = jnp.pad(all_vec, ((0, 0), (0, 0), (0, 5), (0, 0)))
        eb1 = [jnp.broadcast_to(edge_b1[l][None], (8, width)) for l in range(2)]
        nb1 = [jnp.broadcast_to(node_b1[l][None], (8, width)) for l in range(2)]
        nw1 = [jnp.stack(nw[l][:2]) for l in range(2)]

        def chip_sum(pair_a, pair_b):
            return pair_a + swap(pair_b, 1)

        def all_sum(pair_a, pair_b):
            chip = chip_sum(pair_a, pair_b)
            total = chip + swap(chip, 2)[::-1]
            return total, swap(total, 1)

        def own_sum(pair_a, pair_b):
            chip = chip_sum(pair_a, pair_b)
            return chip[0] + swap(chip[1], 2)

        v0, ps, pr = node_project(v_slots, ew[0][1], ew[0][2], eb1[0])
        hid0, nrm0, inv0, e1, sa, sb = edge_forward(
            snd, rcv, x_slots, ps, pr, ew[0][0], ew[0][3], all_vec[0, 0], False, pad_nodes)
        sa, sb = all_sum(sa, sb)
        v1, s0, nhid, nnrm, ninv, ps, pr = node_forward(
            v0, sa, sb, nw1[0], nw[0][2], all_vec[1, 0], nb1[0], ew[1][1], ew[1][2], eb1[1])
        out1 = edge_forward(snd, rcv, [e1], ps, pr, ew[1][0], ew[1][3], all_vec[0, 1], True, pad_nodes)
        hid1, nrm1, inv1 = out1[:3]
        edge_out = to_columns(out1[3:7])
        sa, sb = all_sum(*out1[7:])

        v2, ds, dv, gn1, ndb1 = node_top(v1, sa, sb, [gn_pad] + list(gn_slots[1:]), nw1[1], nw[1][2], all_vec[1, 1], nb1[1])
        node_out = v2[:nodes][None]

        def mine_only(db1):
            lane = lax.broadcasted_iota(jnp.int32, db1.shape, 1)
            return jnp.where(lane // LANES == me, db1, 0.0)

        def edge_grad_sum(pair_a, pair_b):
            own = own_sum(pair_a, pair_b)
            return own + swap_dp(own)

        d_e1, dw1e, dw2t, small, ts, tr = edge_backward(
            snd, rcv, g_slots, [e1], (hid1, nrm1, inv1), ds, ew[1][0], ew[1][3], all_vec[0, 1], True, pad_nodes)
        da, db, ga1, gb1 = proj_backward(ts, tr, v1, ew[1][1], ew[1][2], dw1e, dw2t, small, mine_only(ndb1))
        da, db = all_sum(da, db)
        ds, dv_own, gn0, ndb1 = node_backward(
            dv, da, db, v0, s0, (nhid, nnrm, ninv), nw1[0], nw[0][2], all_vec[1, 0])
        *d_slots, dw1e, dw2t, small, ts, tr = edge_backward(
            snd, rcv, [d_e1], x_slots, (hid0, nrm0, inv0), ds, ew[0][0], ew[0][3], all_vec[0, 0], False, pad_nodes)
        d_edge = to_columns(d_slots)
        da, db, ga0, gb0 = proj_backward(ts, tr, v0, ew[0][1], ew[0][2], dw1e, dw2t, small, mine_only(ndb1))
        d_node = (dv_own + own_sum(da, db))[:nodes].astype(BF16)[None]

        ge = [edge_grad_sum(ga0, gb0), edge_grad_sum(ga1, gb1)]
        gn = [gn0 + swap_dp(gn0), gn1 + swap_dp(gn1)]
        stack = lambda fn: jnp.stack([fn(l) for l in range(2)])
        return (node_out, edge_out, d_node, d_edge,
                stack(lambda l: ge[l][:384].reshape(3, LANES, width)),
                stack(lambda l: ge[l][513]),
                stack(lambda l: ge[l][384:512].T),
                stack(lambda l: ge[l][512, :384].reshape(3, LANES)),
                stack(lambda l: gn[l][:256].reshape(2, LANES, width)),
                stack(lambda l: ge[l][514]),
                stack(lambda l: gn[l][256:384].T),
                stack(lambda l: gn[l][384, :384].reshape(3, LANES)))

    return jax.shard_map(local_step, mesh=mesh, in_specs=in_specs, out_specs=out_specs, check_vma=False)
```

```python
import functools

import jax
import jax.numpy as jnp
from jax import lax
from jax.experimental import pallas as pl
from jax.experimental.pallas import tpu as pltpu
from jax.sharding import PartitionSpec as P

LN_EPS = 1e-5
F32 = jnp.float32
BF16 = jnp.bfloat16
LANES = 128
EDGE_BLK = 256
NODE_BLK = 368
GATHER_UNROLL = 16
ALL = Ellipsis
FULL = (slice(None), slice(None))
VMEM_BYTES = 64 * 2**20 - 2**16


WORK = 4 * 10**9


def wide(val):
    return val.shape[-1]


def slot_views(pair_a, pair_b):
    return pair_a.at[0], pair_b.at[0], pair_a.at[1], pair_b.at[1]


def dot(lhs, rhs):
    return lax.dot_general(lhs, rhs, (((1,), (0,)), ((), ())), preferred_element_type=F32)


def dot_tb(lhs, rhs):
    return lax.dot_general(lhs, rhs, (((1,), (1,)), ((), ())), preferred_element_type=F32)


def dot_ta(lhs, rhs):
    return lax.dot_general(lhs, rhs, (((0,), (0,)), ((), ())), preferred_element_type=F32)


def col(val, slot):
    return val[:, slot * LANES:(slot + 1) * LANES]


def gather_rows(tables, index_refs, base, out_ref, num_rows):
    def step(it, carry):
        for sub in range(GATHER_UNROLL):
            row = it * GATHER_UNROLL + sub
            acc = None
            for table, index_ref in zip(tables, index_refs):
                val = table[pl.ds(pl.multiple_of(index_ref[base + row], 4), 4), :]
                acc = val if acc is None else acc + val
            out_ref[pl.ds(pl.multiple_of(row * 4, 4), 4), :] = acc
        return carry
    lax.fori_loop(0, num_rows // GATHER_UNROLL, step, 0)


def scatter_rows(accs, index_refs, base, src_ref, num_rows, copies, stride):
    def step(it, carry):
        pending = []
        for sub in range(copies):
            row = it * copies + sub
            val = src_ref[pl.ds(pl.multiple_of(row * 4, 4), 4), :]
            for acc, index_ref in zip(accs, index_refs):
                at = pl.multiple_of(index_ref[base + row] + sub * stride, 4)
                pending.append((acc, at, acc[pl.ds(at, 4), :] + val))
        for acc, at, val in pending:
            acc[pl.ds(at, 4), :] = val
        return carry
    lax.fori_loop(0, num_rows // copies, step, 0)


def gather_flat(tables, index_refs, base, out_ref, rows):
    for row in rows:
        acc = None
        for table, index_ref in zip(tables, index_refs):
            val = table[pl.ds(pl.multiple_of(index_ref[base + row], 4), 4), :]
            acc = val if acc is None else acc + val
        out_ref[4 * row:4 * row + 4, :] = acc


def scatter_flat(accs, index_refs, base, src_ref, rows, copies, stride):
    for row in rows[::copies]:
        pending = []
        for sub in range(copies):
            val = src_ref[4 * (row + sub):4 * (row + sub) + 4, :]
            for acc, index_ref in zip(accs, index_refs):
                at = pl.multiple_of(index_ref[base + row + sub] + sub * stride, 4)
                pending.append((acc, at, acc[pl.ds(at, 4), :] + val))
        for acc, at, val in pending:
            acc[pl.ds(at, 4), :] = val


def zero_rows(ref, rows, step_rows):
    def step(it, carry):
        ref[pl.ds(pl.multiple_of(it * step_rows, 8), step_rows), :] = jnp.zeros((step_rows, LANES), F32)
        return carry
    lax.fori_loop(0, rows // step_rows, step, 0)


def row_mean(val):
    return jnp.sum(val, axis=-1, keepdims=True) * (1.0 / val.shape[-1])


def mlp_tail(hidden, w2t, vec_ref):
    act = (hidden * jax.nn.sigmoid(hidden)).astype(BF16)
    out = dot_tb(act, w2t) + vec_ref[0:1, :]
    centered = out - row_mean(out)
    inv_std = lax.rsqrt(row_mean(centered * centered) + LN_EPS)
    normed = centered * inv_std
    message = (normed * vec_ref[1:2, :] + vec_ref[2:3, :]).astype(BF16)
    return act, normed, inv_std, message


def mlp_back(d_message, hidden, normed, inv_std, w2t, vec_ref):
    d_normed = d_message * vec_ref[1:2, :]
    d_out = inv_std * (d_normed - row_mean(d_normed) - normed * row_mean(d_normed * normed))
    d_out_bf = d_out.astype(BF16)
    sig = jax.nn.sigmoid(hidden)
    act = (hidden * sig).astype(BF16)
    d_act = dot(d_out_bf, w2t)
    d_hidden = d_act * (sig * (1.0 + hidden * (1.0 - sig)))
    sums = [jnp.sum(x.reshape(-1, 8, wide(x)), axis=0) for x in (d_out, d_message * normed, d_message, d_hidden)]
    return d_out_bf, act, d_hidden, sums


def add_to(ref, idx, val, first):
    @pl.when(first)
    def _():
        ref[idx] = val

    @pl.when(jnp.logical_not(first))
    def _():
        ref[idx] += val


def call(body, grid, in_specs, out_specs, out_shape, scratch, name, prefetch=0, work=1):
    return pl.pallas_call(
        body,
        out_shape=out_shape,
        grid_spec=pltpu.PrefetchScalarGridSpec(
            num_scalar_prefetch=prefetch, grid=grid, in_specs=in_specs, out_specs=out_specs, scratch_shapes=scratch),
        compiler_params=pltpu.CompilerParams(vmem_limit_bytes=VMEM_BYTES, dimension_semantics=("arbitrary",) * len(grid)),
        cost_estimate=pl.CostEstimate(flops=work * WORK, bytes_accessed=work * WORK // 1000, transcendentals=0),
        name=name)


def rows_spec(blk, width):
    return pl.BlockSpec((blk, width), lambda i, *_: (i, 0))


def whole_spec(shape):
    zeros = (0,) * len(shape)
    return pl.BlockSpec(shape, lambda i, *_: zeros, pipeline_mode=pl.Buffered(1))


def pair_spec(blk):
    return pl.BlockSpec((2, blk, LANES), lambda i, *_: (0, i, 0))


def sds(shape, dtype):
    return jax.ShapeDtypeStruct(shape, dtype)


def edge_fwd_body(n_in, last, pad_nodes, copies, snd_ref, rcv_ref, *refs):
    x_refs = refs[:n_in]
    ps_ref, pr_ref, w1_ref, w2t_ref, vec_ref, hid_ref, nrm_ref, inv_ref = refs[n_in:n_in + 8]
    n_out = 4 if last else 1
    new_refs = refs[n_in + 8:n_in + 8 + n_out]
    sa_ref, sb_ref, gat_ref, msg_ref, acc_ref = refs[n_in + 8 + n_out:]
    step = pl.program_id(0)
    base = step * EDGE_BLK
    stride = 4 * pad_nodes

    last_step = pl.num_programs(0) - 1

    @pl.when(step == 0)
    def _():
        zero_rows(acc_ref, stride * copies, stride // 4)
        msg_ref[ALL] = jnp.zeros(msg_ref.shape, F32)
        gather_rows((ps_ref, pr_ref), (snd_ref, rcv_ref), base, gat_ref, EDGE_BLK)

    x_in = jnp.concatenate([ref[ALL].astype(BF16) for ref in x_refs], axis=-1)
    part = dot(x_in, w1_ref[ALL])
    hidden = jnp.concatenate(
        [col(part, slot) + gat_ref[pl.ds(slot, EDGE_BLK, stride=4), :] for slot in range(4)], axis=-1)
    hid_ref[ALL] = hidden
    scatter_flat((acc_ref,), (rcv_ref,), jnp.maximum(base - EDGE_BLK, 0), msg_ref, range(EDGE_BLK), copies, stride)
    gather_flat((ps_ref, pr_ref), (snd_ref, rcv_ref), jnp.minimum(base + EDGE_BLK, last_step * EDGE_BLK), gat_ref, range(EDGE_BLK))
    _, normed, inv_std, message = mlp_tail(hidden, w2t_ref[ALL], vec_ref)
    nrm_ref[ALL] = normed
    inv_ref[ALL] = jnp.broadcast_to(inv_std, (EDGE_BLK, LANES))
    msg = message.astype(F32)
    new = (x_in.astype(F32) + msg).astype(BF16)
    if last:
        for slot in range(4):
            new_refs[slot][ALL] = col(new, slot).astype(new_refs[slot].dtype)
    else:
        new_refs[0][ALL] = new
    for slot in range(4):
        msg_ref[pl.ds(slot, EDGE_BLK, stride=4), :] = col(msg, slot)

    @pl.when(step == last_step)
    def _():
        scatter_rows((acc_ref,), (rcv_ref,), base, msg_ref, EDGE_BLK, copies, stride)

    @pl.when(step == pl.num_programs(0) - 1)
    def _():
        def fin(it, carry):
            for slot, out in enumerate(slot_views(sa_ref, sb_ref)):
                total = acc_ref[pl.ds(it * (4 * NODE_BLK) + slot, NODE_BLK, stride=4), :]
                for cp in range(1, copies):
                    total = total + acc_ref[pl.ds(it * (4 * NODE_BLK) + slot + cp * stride, NODE_BLK, stride=4), :]
                out[pl.ds(pl.multiple_of(it * NODE_BLK, 8), NODE_BLK), :] = total
            return carry
        lax.fori_loop(0, pad_nodes // NODE_BLK, fin, 0)


def edge_forward(snd, rcv, xs, ps, pr, w1, w2t, vec, last, pad_nodes):
    rows, width = snd.shape[0], w1.shape[0]
    copies = 4
    n_in = len(xs)
    slot_shapes = [sds((rows, LANES), BF16)] + [sds((rows, LANES), F32)] * 3
    new_shapes = slot_shapes if last else [sds((rows, width), BF16)]
    outs = [sds((rows, width), F32), sds((rows, width), F32), sds((rows, LANES), F32)] + new_shapes
    outs += [sds((2, pad_nodes, LANES), F32)] * 2
    in_specs = [rows_spec(EDGE_BLK, wide(x)) for x in xs]
    in_specs += [whole_spec(a.shape) for a in (ps, pr, w1, w2t, vec)]
    out_specs = [rows_spec(EDGE_BLK, wide(o)) for o in outs[:-2]] + [whole_spec(o.shape) for o in outs[-2:]]
    scratch = [pltpu.VMEM((4 * EDGE_BLK, LANES), F32), pltpu.VMEM((4 * EDGE_BLK, LANES), F32),
               pltpu.VMEM((copies * 4 * pad_nodes, LANES), F32)]
    return call(functools.partial(edge_fwd_body, n_in, last, pad_nodes, copies), (rows // EDGE_BLK,), in_specs, out_specs,
                outs, scratch, "edge_fwd", prefetch=2, work=12)(snd, rcv, *xs, ps, pr, w1, w2t, vec)


def edge_bwd_body(n_in, last, pad_nodes, copies, snd_ref, rcv_ref, *refs):
    n_g = 4 if last else 1
    g_refs = refs[:n_g]
    x_refs = refs[n_g:n_g + n_in]
    hid_ref, nrm_ref, inv_ref, ds_ref, w1_ref, w2t_ref, vec_ref = refs[n_g + n_in:n_g + n_in + 7]
    rest = refs[n_g + n_in + 7:]
    n_out = 1 if last else 4
    d_refs = rest[:n_out]
    dw1_ref, dw2t_ref, small_ref, ts_ref, tr_ref, gat_ref, dh_ref, accs_ref, accr_ref, sums_ref = rest[n_out:]
    step = pl.program_id(0)
    base = step * EDGE_BLK
    stride = 4 * pad_nodes
    last_step = pl.num_programs(0) - 1

    @pl.when(step == 0)
    def _():
        zero_rows(accs_ref, stride * copies, stride // 4)
        zero_rows(accr_ref, stride * copies, stride // 4)
        for ref in (dh_ref, dw1_ref, dw2t_ref, sums_ref):
            ref[ALL] = jnp.zeros(ref.shape, F32)
        gather_rows((ds_ref,), (rcv_ref,), base, gat_ref, EDGE_BLK)

    d_edge = jnp.concatenate([ref[ALL].astype(F32) for ref in g_refs], axis=-1)
    d_message = jnp.concatenate(
        [col(d_edge, slot) + gat_ref[pl.ds(slot, EDGE_BLK, stride=4), :] for slot in range(4)], axis=-1)
    scatter_flat((accs_ref, accr_ref), (snd_ref, rcv_ref), jnp.maximum(base - EDGE_BLK, 0), dh_ref, range(EDGE_BLK), copies, stride)
    gather_flat((ds_ref,), (rcv_ref,), jnp.minimum(base + EDGE_BLK, last_step * EDGE_BLK), gat_ref, range(EDGE_BLK))
    d_out_bf, act, d_hidden, sums = mlp_back(
        d_message, hid_ref[ALL], nrm_ref[ALL], inv_ref[:, 0:1], w2t_ref[ALL], vec_ref)
    d_hidden_bf = d_hidden.astype(BF16)
    x_in = jnp.concatenate([ref[ALL].astype(BF16) for ref in x_refs], axis=-1)
    dw2t_ref[ALL] += dot_ta(d_out_bf, act)
    dw1_ref[ALL] += dot_ta(x_in, d_hidden_bf)
    sums_ref[ALL] += jnp.concatenate(sums, axis=0)
    d_x = (d_edge + dot_tb(d_hidden_bf, w1_ref[ALL])).astype(BF16)
    if last:
        d_refs[0][ALL] = d_x
    else:
        for slot in range(4):
            d_refs[slot][ALL] = col(d_x, slot).astype(d_refs[slot].dtype)
    for slot in range(4):
        dh_ref[pl.ds(slot, EDGE_BLK, stride=4), :] = col(d_hidden, slot)

    @pl.when(step == last_step)
    def _():
        scatter_rows((accs_ref, accr_ref), (snd_ref, rcv_ref), base, dh_ref, EDGE_BLK, copies, stride)
        total = [jnp.sum(sums_ref[8 * k:8 * k + 8, :], axis=0, keepdims=True) for k in range(4)]
        small_ref[ALL] = jnp.concatenate(total + [jnp.zeros((4, wide(small_ref)), F32)], axis=0)

        def fin(it, carry):
            for acc_ref, out_ref in ((accs_ref, ts_ref), (accr_ref, tr_ref)):
                for slot in range(4):
                    total = acc_ref[pl.ds(it * (4 * NODE_BLK) + slot, NODE_BLK, stride=4), :]
                    for cp in range(1, copies):
                        total = total + acc_ref[pl.ds(it * (4 * NODE_BLK) + slot + cp * stride, NODE_BLK, stride=4), :]
                    out_ref[pl.ds(pl.multiple_of(it * NODE_BLK, 16), NODE_BLK),
                            slot * LANES:(slot + 1) * LANES] = total.astype(BF16)
            return carry
        lax.fori_loop(0, pad_nodes // NODE_BLK, fin, 0)


def edge_backward(snd, rcv, gs, xs, saved, ds, w1, w2t, vec, last, pad_nodes):
    rows, width = snd.shape[0], w1.shape[0]
    copies = 2
    hid, nrm, inv = saved
    slot_shapes = [sds((rows, LANES), BF16)] + [sds((rows, LANES), F32)] * 3
    d_shapes = [sds((rows, width), BF16)] if last else slot_shapes
    tail = [sds((width, width), F32), sds((width, width), F32), sds((8, width), F32),
            sds((pad_nodes, width), BF16), sds((pad_nodes, width), BF16)]
    ins = list(gs) + list(xs) + [hid, nrm, inv]
    in_specs = [rows_spec(EDGE_BLK, wide(x)) for x in ins] + [whole_spec(a.shape) for a in (ds, w1, w2t, vec)]
    out_specs = [rows_spec(EDGE_BLK, wide(o)) for o in d_shapes] + [whole_spec(o.shape) for o in tail]
    scratch = [pltpu.VMEM((4 * EDGE_BLK, LANES), F32), pltpu.VMEM((4 * EDGE_BLK, LANES), F32),
               pltpu.VMEM((copies * 4 * pad_nodes, LANES), F32), pltpu.VMEM((copies * 4 * pad_nodes, LANES), F32),
               pltpu.VMEM((4 * 8, width), F32)]
    return call(functools.partial(edge_bwd_body, len(xs), last, pad_nodes, copies), (rows // EDGE_BLK,), in_specs, out_specs,
                d_shapes + tail, scratch, "edge_bwd", prefetch=2, work=20)(snd, rcv, *ins, ds, w1, w2t, vec)


def proj_bwd_body(ts_ref, tr_ref, v_ref, w1s_ref, w1r_ref, dw1e_ref, dw2t_ref, small_ref, node_b1_ref,
                  da_ref, db_ref, ga_ref, gb_ref, acc_s, acc_r):
    step = pl.program_id(0)
    first = step == 0
    d_v = dot_tb(ts_ref[ALL], w1s_ref[ALL]) + dot_tb(tr_ref[ALL], w1r_ref[ALL])
    for slot, out in enumerate(slot_views(da_ref, db_ref)):
        out[ALL] = col(d_v, slot)
    add_to(acc_s, FULL, dot_ta(v_ref[ALL], ts_ref[ALL]), first)
    add_to(acc_r, FULL, dot_ta(v_ref[ALL], tr_ref[ALL]), first)

    @pl.when(step == pl.num_programs(0) - 1)
    def _():
        for slot, out in enumerate(slot_views(ga_ref, gb_ref)):
            rows = slice(slot * LANES, (slot + 1) * LANES)
            for part, src in enumerate((dw1e_ref, acc_s, acc_r, dw2t_ref)):
                out[part * LANES:(part + 1) * LANES, :] = src[rows, :]
            vec_row = jnp.concatenate(
                [small_ref[k:k + 1, rows] for k in range(3)] + [jnp.zeros((1, LANES), F32)], axis=-1)
            out[512:520, :] = jnp.concatenate(
                [vec_row, small_ref[3:4, :], node_b1_ref[0:1, :], jnp.zeros((5, wide(vec_row)), F32)], axis=0)


def proj_backward(ts, tr, v_full, w1s, w1r, dw1e, dw2t, small, node_b1):
    nodes, width = v_full.shape
    ins = [ts, tr, v_full, w1s, w1r, dw1e, dw2t, small, node_b1]
    outs = [sds((2, nodes, LANES), F32)] * 2 + [sds((2, width + 8, width), F32)] * 2
    in_specs = [rows_spec(NODE_BLK, width)] * 3 + [whole_spec(a.shape) for a in ins[3:]]
    out_specs = [pair_spec(NODE_BLK)] * 2 + [whole_spec(outs[2].shape)] * 2
    scratch = [pltpu.VMEM((width, width), F32)] * 2
    return call(proj_bwd_body, (nodes // NODE_BLK,), in_specs, out_specs, outs, scratch, "proj_bwd")(*ins)


def write_table(ref, val):
    for slot in range(4):
        ref[pl.ds(slot, NODE_BLK, stride=4), :] = col(val, slot)


def node_proj_body(v0_ref, v1_ref, v2_ref, v3_ref, w1s_ref, w1r_ref, b1_ref, v_ref, ps_ref, pr_ref):
    v_in = jnp.concatenate([ref[ALL].astype(BF16) for ref in (v0_ref, v1_ref, v2_ref, v3_ref)], axis=-1)
    v_ref[ALL] = v_in
    write_table(ps_ref, dot(v_in, w1s_ref[ALL]) + b1_ref[0:1, :])
    write_table(pr_ref, dot(v_in, w1r_ref[ALL]))


def node_project(vs, w1s, w1r, b1):
    nodes, width = vs[0].shape[0], w1s.shape[0]
    in_specs = [rows_spec(NODE_BLK, LANES)] * 4 + [whole_spec(a.shape) for a in (w1s, w1r, b1)]
    outs = [sds((nodes, width), BF16), sds((4 * nodes, LANES), F32), sds((4 * nodes, LANES), F32)]
    out_specs = [rows_spec(NODE_BLK, width)] + [rows_spec(4 * NODE_BLK, LANES)] * 2
    return call(node_proj_body, (nodes // NODE_BLK,), in_specs, out_specs, outs, [], "node_proj")(
        *vs, w1s, w1r, b1)


def read_pairs(a_ref, b_ref):
    return jnp.concatenate([a_ref[0], b_ref[0], a_ref[1], b_ref[1]], axis=-1)


def node_fwd_body(v_ref, sa_ref, sb_ref, w1_ref, w2t_ref, vec_ref, b1_ref, w1s_ref, w1r_ref, eb1_ref,
                  new_ref, s_ref, hid_ref, nrm_ref, inv_ref, ps_ref, pr_ref):
    v_in = v_ref[ALL]
    s_in = read_pairs(sa_ref, sb_ref).astype(BF16)
    s_ref[ALL] = s_in
    hidden = dot(v_in, w1_ref[0]) + dot(s_in, w1_ref[1]) + b1_ref[0:1, :]
    hid_ref[ALL] = hidden
    _, normed, inv_std, message = mlp_tail(hidden, w2t_ref[ALL], vec_ref)
    nrm_ref[ALL] = normed
    inv_ref[ALL] = jnp.broadcast_to(inv_std, (NODE_BLK, LANES))
    new = (v_in.astype(F32) + message.astype(F32)).astype(BF16)
    new_ref[ALL] = new
    write_table(ps_ref, dot(new, w1s_ref[ALL]) + eb1_ref[0:1, :])
    write_table(pr_ref, dot(new, w1r_ref[ALL]))


def node_forward(v_in, sa, sb, w1, w2t, vec, b1, w1s, w1r, eb1):
    nodes, width = v_in.shape
    in_specs = [rows_spec(NODE_BLK, width), pair_spec(NODE_BLK), pair_spec(NODE_BLK)]
    in_specs += [whole_spec(a.shape) for a in (w1, w2t, vec, b1, w1s, w1r, eb1)]
    outs = [sds((nodes, width), BF16), sds((nodes, width), BF16), sds((nodes, width), F32), sds((nodes, width), F32),
            sds((nodes, LANES), F32), sds((4 * nodes, LANES), F32), sds((4 * nodes, LANES), F32)]
    out_specs = [rows_spec(NODE_BLK, wide(o)) for o in outs[:5]] + [rows_spec(4 * NODE_BLK, LANES)] * 2
    return call(node_fwd_body, (nodes // NODE_BLK,), in_specs, out_specs, outs, [], "node_fwd")(
        v_in, sa, sb, w1, w2t, vec, b1, w1s, w1r, eb1)


def node_grads(first, d_message, v_in, s_in, hidden, normed, inv_std, w1_ref, w2t_ref, vec_ref, ds_ref, gn_ref, db1_ref):
    d_out_bf, act, d_hidden, sums = mlp_back(d_message, hidden, normed, inv_std, w2t_ref[ALL], vec_ref)
    d_hidden_bf = d_hidden.astype(BF16)
    write_table(ds_ref, dot_tb(d_hidden_bf, w1_ref[1]))
    whole = slice(None)
    add_to(gn_ref, (slice(0, LANES), whole), dot_ta(col(v_in, 0), d_hidden_bf), first)
    add_to(gn_ref, (slice(LANES, 2 * LANES), whole), dot_ta(col(s_in, 0), d_hidden_bf), first)
    add_to(gn_ref, (slice(2 * LANES, 3 * LANES), whole), dot_ta(col(d_out_bf, 0), act), first)
    add_to(gn_ref, (slice(3 * LANES, 3 * LANES + 8), whole),
           jnp.concatenate([col(x, 0) for x in sums[:3]] + [jnp.zeros((8, LANES), F32)], axis=-1), first)
    add_to(db1_ref, (whole, whole), sums[3], first)
    return dot_tb(d_hidden_bf, w1_ref[0])


def node_top_body(v_ref, sa_ref, sb_ref, g0_ref, g1_ref, g2_ref, g3_ref, w1_ref, w2t_ref, vec_ref, b1_ref,
                  new_ref, ds_ref, dv_ref, gn_ref, db1_ref):
    first = pl.program_id(0) == 0
    v_in = v_ref[ALL]
    s_in = read_pairs(sa_ref, sb_ref).astype(BF16)
    hidden = dot(v_in, w1_ref[0]) + dot(s_in, w1_ref[1]) + b1_ref[0:1, :]
    _, normed, inv_std, message = mlp_tail(hidden, w2t_ref[ALL], vec_ref)
    new_ref[ALL] = (col(v_in, 0).astype(F32) + col(message, 0).astype(F32)).astype(BF16)
    d_new = jnp.concatenate([ref[ALL].astype(F32) for ref in (g0_ref, g1_ref, g2_ref, g3_ref)], axis=-1)
    dv_ref[ALL] = d_new + node_grads(
        first, d_new, v_in, s_in, hidden, normed, inv_std, w1_ref, w2t_ref, vec_ref, ds_ref, gn_ref, db1_ref)


def node_top(v_in, sa, sb, gs, w1, w2t, vec, b1):
    nodes, width = v_in.shape
    in_specs = [rows_spec(NODE_BLK, width), pair_spec(NODE_BLK), pair_spec(NODE_BLK)] + [rows_spec(NODE_BLK, LANES)] * 4
    in_specs += [whole_spec(a.shape) for a in (w1, w2t, vec, b1)]
    outs = [sds((nodes, LANES), BF16), sds((4 * nodes, LANES), F32), sds((nodes, width), F32),
            sds((3 * LANES + 8, width), F32), sds((8, width), F32)]
    out_specs = [rows_spec(NODE_BLK, LANES), rows_spec(4 * NODE_BLK, LANES), rows_spec(NODE_BLK, width),
                 whole_spec(outs[3].shape), whole_spec(outs[4].shape)]
    return call(node_top_body, (nodes // NODE_BLK,), in_specs, out_specs, outs, [], "node_top")(
        v_in, sa, sb, *gs, w1, w2t, vec, b1)


def node_bwd_body(dv_ref, ta_ref, tb_ref, v_ref, s_ref, hid_ref, nrm_ref, inv_ref, w1_ref, w2t_ref, vec_ref,
                  ds_ref, dvo_ref, gn_ref, db1_ref):
    first = pl.program_id(0) == 0
    d_new = (dv_ref[ALL] + read_pairs(ta_ref, tb_ref)).astype(BF16).astype(F32)
    d_v = node_grads(first, d_new, v_ref[ALL], s_ref[ALL], hid_ref[ALL], nrm_ref[ALL], inv_ref[:, 0:1],
                     w1_ref, w2t_ref, vec_ref, ds_ref, gn_ref, db1_ref)
    dvo_ref[ALL] = col(d_new, 0) + col(d_v, 0)


def node_backward(dv, ta, tb, v_in, s_in, saved, w1, w2t, vec):
    nodes, width = v_in.shape
    ins = [dv, ta, tb, v_in, s_in, *saved]
    in_specs = [rows_spec(NODE_BLK, width), pair_spec(NODE_BLK), pair_spec(NODE_BLK)]
    in_specs += [rows_spec(NODE_BLK, wide(a)) for a in ins[3:]] + [whole_spec(a.shape) for a in (w1, w2t, vec)]
    outs = [sds((4 * nodes, LANES), F32), sds((nodes, LANES), F32), sds((3 * LANES + 8, width), F32), sds((8, width), F32)]
    out_specs = [rows_spec(4 * NODE_BLK, LANES), rows_spec(NODE_BLK, LANES), whole_spec(outs[2].shape),
                 whole_spec(outs[3].shape)]
    return call(node_bwd_body, (nodes // NODE_BLK,), in_specs, out_specs, outs, [], "node_bwd")(
        *ins, w1, w2t, vec)


def to_slots_body(limit, me_ref, x_ref, *out_refs):
    part, slot = pl.program_id(0), pl.program_id(1)
    blk = x_ref.shape[0]
    at = ((me_ref[0] ^ slot) * pl.num_programs(0) + part) * blk
    row = lax.broadcasted_iota(jnp.int32, x_ref.shape, 0) + at
    val = jnp.where(row < limit, x_ref[ALL].astype(F32), 0.0)
    for k, out in enumerate(out_refs):
        @pl.when(slot == k)
        def _():
            out[ALL] = val.astype(out.dtype)


def to_slots(me, val, rows):
    limit, parts = val.shape[0], 2
    blk = rows // parts
    outs = [sds((rows, LANES), BF16)] + [sds((rows, LANES), F32)] * 3
    return call(functools.partial(to_slots_body, limit), (parts, 4),
                [pl.BlockSpec((blk, LANES), lambda r, d, me: ((me[0] ^ d) * parts + r, 0))],
                [pl.BlockSpec((blk, LANES), lambda r, d, me: (r, 0))] * 4, outs, [], "to_slots", prefetch=1)(me, val)


def from_slots_body(me_ref, *refs):
    out_ref = refs[-1]
    for k, ref in enumerate(refs[:-1]):
        @pl.when(pl.program_id(1) == k)
        def _():
            out_ref[ALL] = ref[ALL].astype(BF16)


def from_slots(me, slots, limit):
    rows, parts = slots[0].shape[0], 2
    blk = rows // parts
    return call(from_slots_body, (parts, 4), [pl.BlockSpec((blk, LANES), lambda r, d, me: (r, 0))] * 4,
                pl.BlockSpec((blk, LANES), lambda r, d, me: ((me[0] ^ d) * parts + r, 0)), sds((limit, LANES), BF16), [],
                "from_slots", prefetch=1)(me, *slots)


def unpack_body(starts, *refs):
    slots, outs = refs[:4], refs[4:]
    for at, out in zip(starts, outs):
        for k, ref in enumerate(slots):
            out[k * LANES:(k + 1) * LANES, :] = ref[at:at + LANES, :].astype(BF16)


def unpack_weights(slots, starts):
    width = wide(slots[0])
    outs = [sds((4 * LANES, width), BF16)] * len(starts)
    return call(functools.partial(unpack_body, starts), (1,), [whole_spec(s.shape) for s in slots],
                [whole_spec(o.shape) for o in outs], outs, [], "unpack")(*slots)


def solution(mesh):
    lat_spec = P('dp', None, 'tp')
    first_spec = P(None, None, 'tp', None)
    col_spec = P(None, None, 'tp')
    param_specs = (first_spec, P(), col_spec, col_spec, first_spec, P(), col_spec, col_spec)
    in_specs = (lat_spec, lat_spec, P(), P(), lat_spec, lat_spec) + param_specs
    out_specs = (lat_spec, lat_spec, lat_spec, lat_spec) + param_specs
    tp = mesh.shape['tp']

    def swap(val, mask):
        return lax.ppermute(val, 'tp', [(i, i ^ mask) for i in range(tp)])

    def swap_dp(val):
        return lax.ppermute(val, 'dp', [(0, 1), (1, 0)])

    def slots_of(val):
        far = swap(val, 2)
        return val, swap(val, 1), far, swap(far, 1)

    def local_step(node_lat, edge_lat, senders, receivers, grad_node, grad_edge,
                   edge_w1, edge_b1, edge_w2, edge_vec, node_w1, node_b1, node_w2, node_vec):
        me = lax.axis_index('tp')
        _, nodes, _ = node_lat.shape
        _, edges, _ = edge_lat.shape
        width = wide(edge_b1)
        rows = -(-edges // (tp * EDGE_BLK)) * EDGE_BLK
        pad_nodes = (nodes // NODE_BLK + 1) * NODE_BLK

        me_ref = me.astype(jnp.int32)[None]

        def to_rows(val):
            blocks = to_slots(me_ref, val, rows)
            return [blocks[0]] + [swap(blocks[d], d) for d in range(1, tp)]

        def to_columns(slots):
            return from_slots(me_ref, [slots[0]] + [swap(slots[d], d) for d in range(1, tp)], edges)[None]

        def my_index(ids):
            padded = jnp.pad(ids, (0, tp * rows - edges), constant_values=nodes)
            return lax.dynamic_slice(padded, (me * rows,), (rows,)) * 4

        snd, rcv = my_index(senders), my_index(receivers)

        def pack(l, w1, w2):
            return jnp.concatenate([w1[l].reshape(-1, width), w2[l].T], axis=0).astype(F32)

        vecs = jnp.concatenate([edge_vec.reshape(-1), node_vec.reshape(-1)]).reshape(-1, width)
        vecs = jnp.pad(vecs, ((0, 8 - vecs.shape[0]), (0, 0)))
        group_a = jnp.concatenate([pack(0, edge_w1, edge_w2), vecs], axis=0)
        group_b = jnp.concatenate([pack(0, node_w1, node_w2), pack(1, edge_w1, edge_w2), pack(1, node_w1, node_w2)], axis=0)
        v_pad = jnp.pad(node_lat[0], ((0, pad_nodes - nodes), (0, 0)))
        v_slots = slots_of(v_pad.astype(F32))
        slots_a = slots_of(group_a)
        x_slots = to_rows(edge_lat[0])
        slots_b = slots_of(group_b)
        g_slots = to_rows(grad_edge[0])
        gn_pad = jnp.pad(grad_node[0], ((0, pad_nodes - nodes), (0, 0)))
        gn_slots = slots_of(gn_pad.astype(F32))

        mats_a = unpack_weights(slots_a, (0, 128, 256, 384))
        mats_b = unpack_weights(slots_b, tuple(range(0, 1280, 128)))
        ew, nw = [mats_a, mats_b[3:7]], [mats_b[:3], mats_b[7:]]
        all_vec = jnp.stack([s[512:515].reshape(2, 2, 3, LANES) for s in slots_a], axis=3).reshape(2, 2, 3, width)
        all_vec = jnp.pad(all_vec, ((0, 0), (0, 0), (0, 5), (0, 0)))
        eb1 = [jnp.broadcast_to(edge_b1[l][None], (8, width)) for l in range(2)]
        nb1 = [jnp.broadcast_to(node_b1[l][None], (8, width)) for l in range(2)]
        nw1 = [jnp.stack(nw[l][:2]) for l in range(2)]

        def chip_sum(pair_a, pair_b):
            return pair_a + swap(pair_b, 1)

        def all_sum(pair_a, pair_b):
            chip = chip_sum(pair_a, pair_b)
            total = chip + swap(chip, 2)[::-1]
            return total, swap(total, 1)

        def own_sum(pair_a, pair_b):
            chip = chip_sum(pair_a, pair_b)
            return chip[0] + swap(chip[1], 2)

        v0, ps, pr = node_project(v_slots, ew[0][1], ew[0][2], eb1[0])
        hid0, nrm0, inv0, e1, sa, sb = edge_forward(
            snd, rcv, x_slots, ps, pr, ew[0][0], ew[0][3], all_vec[0, 0], False, pad_nodes)
        sa, sb = all_sum(sa, sb)
        v1, s0, nhid, nnrm, ninv, ps, pr = node_forward(
            v0, sa, sb, nw1[0], nw[0][2], all_vec[1, 0], nb1[0], ew[1][1], ew[1][2], eb1[1])
        out1 = edge_forward(snd, rcv, [e1], ps, pr, ew[1][0], ew[1][3], all_vec[0, 1], True, pad_nodes)
        hid1, nrm1, inv1 = out1[:3]
        edge_out = to_columns(out1[3:7])
        sa, sb = all_sum(*out1[7:])

        v2, ds, dv, gn1, ndb1 = node_top(v1, sa, sb, [gn_pad] + list(gn_slots[1:]), nw1[1], nw[1][2], all_vec[1, 1], nb1[1])
        node_out = v2[:nodes][None]

        def mine_only(db1):
            lane = lax.broadcasted_iota(jnp.int32, db1.shape, 1)
            return jnp.broadcast_to(jnp.where(lane // LANES == me, db1, 0.0).sum(axis=0), db1.shape)

        def edge_grad_sum(pair_a, pair_b):
            own = own_sum(pair_a, pair_b)
            return own + swap_dp(own)

        d_e1, dw1e, dw2t, small, ts, tr = edge_backward(
            snd, rcv, g_slots, [e1], (hid1, nrm1, inv1), ds, ew[1][0], ew[1][3], all_vec[0, 1], True, pad_nodes)
        da, db, ga1, gb1 = proj_backward(ts, tr, v1, ew[1][1], ew[1][2], dw1e, dw2t, small, mine_only(ndb1))
        da, db = all_sum(da, db)
        ds, dv_own, gn0, ndb1 = node_backward(
            dv, da, db, v0, s0, (nhid, nnrm, ninv), nw1[0], nw[0][2], all_vec[1, 0])
        *d_slots, dw1e, dw2t, small, ts, tr = edge_backward(
            snd, rcv, [d_e1], x_slots, (hid0, nrm0, inv0), ds, ew[0][0], ew[0][3], all_vec[0, 0], False, pad_nodes)
        d_edge = to_columns(d_slots)
        da, db, ga0, gb0 = proj_backward(ts, tr, v0, ew[0][1], ew[0][2], dw1e, dw2t, small, mine_only(ndb1))
        d_node = (dv_own + own_sum(da, db))[:nodes].astype(BF16)[None]

        ge = [edge_grad_sum(ga0, gb0), edge_grad_sum(ga1, gb1)]
        gn = [gn0 + swap_dp(gn0), gn1 + swap_dp(gn1)]
        stack = lambda fn: jnp.stack([fn(l) for l in range(2)])
        return (node_out, edge_out, d_node, d_edge,
                stack(lambda l: ge[l][:384].reshape(3, LANES, width)),
                stack(lambda l: ge[l][513]),
                stack(lambda l: ge[l][384:512].T),
                stack(lambda l: ge[l][512, :384].reshape(3, LANES)),
                stack(lambda l: gn[l][:256].reshape(2, LANES, width)),
                stack(lambda l: ge[l][514]),
                stack(lambda l: gn[l][256:384].T),
                stack(lambda l: gn[l][384:, :384].sum(axis=0).reshape(3, LANES)))

    return jax.shard_map(local_step, mesh=mesh, in_specs=in_specs, out_specs=out_specs, check_vma=False)
```

```python
import functools
from typing import Any, NamedTuple

import jax
import jax.numpy as jnp
from jax import lax
from jax.experimental import pallas as pl
from jax.experimental.pallas import tpu as pltpu
from jax.sharding import PartitionSpec as P


LN_EPS = 1e-5
F32 = jnp.float32
BF16 = jnp.bfloat16
LANES = 128
EDGE_BLK = 256
NODE_BLK = 368
GATHER_UNROLL = 16
ALL = Ellipsis
FULL = (slice(None), slice(None))
VMEM_BYTES = 64 * 2**20 - 2**16


WORK = 4 * 10**9


def wide(val):
    return val.shape[-1]


def slot_views(pair_a, pair_b):
    return pair_a.at[0], pair_b.at[0], pair_a.at[1], pair_b.at[1]


def dot(lhs, rhs):
    return lax.dot_general(lhs, rhs, (((1,), (0,)), ((), ())), preferred_element_type=F32)


def dot_tb(lhs, rhs):
    return lax.dot_general(lhs, rhs, (((1,), (1,)), ((), ())), preferred_element_type=F32)


def dot_ta(lhs, rhs):
    return lax.dot_general(lhs, rhs, (((0,), (0,)), ((), ())), preferred_element_type=F32)


def col(val, slot):
    return val[:, slot * LANES:(slot + 1) * LANES]


def gather_rows(tables, index_refs, base, out_ref, num_rows):
    def step(it, carry):
        for sub in range(GATHER_UNROLL):
            row = it * GATHER_UNROLL + sub
            acc = None
            for table, index_ref in zip(tables, index_refs):
                val = table[pl.ds(pl.multiple_of(index_ref[base + row], 4), 4), :]
                acc = val if acc is None else acc + val
            out_ref[pl.ds(pl.multiple_of(row * 4, 4), 4), :] = acc
        return carry

    lax.fori_loop(0, num_rows // GATHER_UNROLL, step, 0)


def scatter_rows(accs, index_refs, base, src_ref, num_rows, copies, stride):
    def step(it, carry):
        pending = []
        for sub in range(copies):
            row = it * copies + sub
            val = src_ref[pl.ds(pl.multiple_of(row * 4, 4), 4), :]
            for acc, index_ref in zip(accs, index_refs):
                at = pl.multiple_of(index_ref[base + row] + sub * stride, 4)
                pending.append((acc, at, acc[pl.ds(at, 4), :] + val))
        for acc, at, val in pending:
            acc[pl.ds(at, 4), :] = val
        return carry

    lax.fori_loop(0, num_rows // copies, step, 0)


def gather_flat(tables, index_refs, base, out_ref, rows):
    for row in rows:
        acc = None
        for table, index_ref in zip(tables, index_refs):
            val = table[pl.ds(pl.multiple_of(index_ref[base + row], 4), 4), :]
            acc = val if acc is None else acc + val
        out_ref[4 * row:4 * row + 4, :] = acc


def scatter_flat(accs, index_refs, base, src_ref, rows, copies, stride):
    for row in rows[::copies]:
        pending = []
        for sub in range(copies):
            val = src_ref[4 * (row + sub):4 * (row + sub) + 4, :]
            for acc, index_ref in zip(accs, index_refs):
                at = pl.multiple_of(index_ref[base + row + sub] + sub * stride, 4)
                pending.append((acc, at, acc[pl.ds(at, 4), :] + val))
        for acc, at, val in pending:
            acc[pl.ds(at, 4), :] = val


def zero_rows(ref, rows, step_rows):
    def step(it, carry):
        ref[pl.ds(pl.multiple_of(it * step_rows, 8), step_rows), :] = jnp.zeros((step_rows, LANES), F32)
        return carry

    lax.fori_loop(0, rows // step_rows, step, 0)


def row_mean(val):
    return jnp.sum(val, axis=-1, keepdims=True) * (1.0 / val.shape[-1])


def mlp_tail(hidden, w2t, vec_ref):
    act = (hidden * jax.nn.sigmoid(hidden)).astype(BF16)
    out = dot_tb(act, w2t) + vec_ref[0:1, :]
    centered = out - row_mean(out)
    inv_std = lax.rsqrt(row_mean(centered * centered) + LN_EPS)
    normed = centered * inv_std
    message = (normed * vec_ref[1:2, :] + vec_ref[2:3, :]).astype(BF16)
    return act, normed, inv_std, message


def mlp_back(d_message, hidden, normed, inv_std, w2t, vec_ref):
    d_normed = d_message * vec_ref[1:2, :]
    d_out = inv_std * (d_normed - row_mean(d_normed) - normed * row_mean(d_normed * normed))
    d_out_bf = d_out.astype(BF16)
    sig = jax.nn.sigmoid(hidden)
    act = (hidden * sig).astype(BF16)
    d_act = dot(d_out_bf, w2t)
    d_hidden = d_act * (sig * (1.0 + hidden * (1.0 - sig)))
    sums = [jnp.sum(x.reshape(-1, 8, wide(x)), axis=0) for x in (d_out, d_message * normed, d_message, d_hidden)]
    return d_out_bf, act, d_hidden, sums


def add_to(ref, idx, val, first):
    @pl.when(first)
    def _():
        ref[idx] = val

    @pl.when(jnp.logical_not(first))
    def _():
        ref[idx] += val


def call(body, grid, in_specs, out_specs, out_shape, scratch, prefetch=0, work=1):
    return pl.pallas_call(
        body,
        out_shape=out_shape,
        grid_spec=pltpu.PrefetchScalarGridSpec(
            num_scalar_prefetch=prefetch, grid=grid, in_specs=in_specs, out_specs=out_specs, scratch_shapes=scratch),
        compiler_params=pltpu.CompilerParams(vmem_limit_bytes=VMEM_BYTES, dimension_semantics=("arbitrary",) * len(grid)),
        cost_estimate=pl.CostEstimate(flops=work * WORK, bytes_accessed=work * WORK // 1000, transcendentals=0))


def rows_spec(blk, width):
    return pl.BlockSpec((blk, width), lambda i, *_: (i, 0))


def whole_spec(shape):
    zeros = (0,) * len(shape)
    return pl.BlockSpec(shape, lambda i, *_: zeros, pipeline_mode=pl.Buffered(1))


def pair_spec(blk):
    return pl.BlockSpec((2, blk, LANES), lambda i, *_: (0, i, 0))


def in_part(lo, num):
    step = pl.program_id(0)
    return jnp.logical_and(step >= lo, step < lo + num)


def part_specs(cuts):
    lows = [sum(cuts[:k]) for k in range(len(cuts))]
    return [pl.BlockSpec((EDGE_BLK, LANES), lambda i, *_, lo=lo, num=num: (jnp.clip(i - lo, 0, num - 1), 0))
            for lo, num in zip(lows, cuts)]


def sds(shape, dtype):
    return jax.ShapeDtypeStruct(shape, dtype)


def edge_fwd_body(n_in, cuts, pad_nodes, copies, snd_ref, rcv_ref, *refs):
    x_refs = refs[:n_in]
    ps_ref, pr_ref, w1_ref, w2t_ref, vec_ref, hid_ref, nrm_ref, inv_ref = refs[n_in:n_in + 8]
    n_out = 2 + 2 * len(cuts) if cuts else 1
    new_refs = refs[n_in + 8:n_in + 8 + n_out]
    sa_ref, sb_ref, gat_ref, msg_ref, acc_ref, far_ref = refs[n_in + 8 + n_out:]
    step = pl.program_id(0)
    base = step * EDGE_BLK
    stride = 4 * pad_nodes

    last_step = pl.num_programs(0) - 1

    @pl.when(step == 0)
    def _():
        zero_rows(acc_ref, stride * copies, stride // 4)
        msg_ref[ALL] = jnp.zeros(msg_ref.shape, F32)
        gather_rows((ps_ref, pr_ref), (snd_ref, rcv_ref), base, gat_ref, EDGE_BLK)

    x_in = jnp.concatenate([ref[ALL].astype(BF16) for ref in x_refs], axis=-1)
    part = dot(x_in, w1_ref[ALL])
    hidden = jnp.concatenate(
        [col(part, slot) + gat_ref[pl.ds(slot, EDGE_BLK, stride=4), :] for slot in range(4)], axis=-1)
    hid_ref[ALL] = hidden
    scatter_flat((acc_ref,), (rcv_ref,), jnp.maximum(base - EDGE_BLK, 0), msg_ref, range(EDGE_BLK), copies, stride)
    gather_flat((ps_ref, pr_ref), (snd_ref, rcv_ref), jnp.minimum(base + EDGE_BLK, last_step * EDGE_BLK), gat_ref, range(EDGE_BLK))
    _, normed, inv_std, message = mlp_tail(hidden, w2t_ref[ALL], vec_ref)
    nrm_ref[ALL] = normed
    inv_ref[ALL] = jnp.broadcast_to(inv_std, (EDGE_BLK, LANES))
    msg = message.astype(F32)
    new = (x_in.astype(F32) + msg).astype(BF16)
    if cuts:
        new_refs[0][ALL] = col(new, 0)
        new_refs[1][ALL] = col(new, 1).astype(F32)
        far_ref[ALL] = new[:, 2 * LANES:].astype(F32)
        lo = 0
        for num, ref2, ref3 in zip(cuts, new_refs[2:], new_refs[2 + len(cuts):]):
            @pl.when(in_part(lo, num))
            def _():
                ref2[ALL] = col(far_ref, 0)
                ref3[ALL] = col(far_ref, 1)

            lo += num
    else:
        new_refs[0][ALL] = new
    for slot in range(4):
        msg_ref[pl.ds(slot, EDGE_BLK, stride=4), :] = col(msg, slot)

    @pl.when(step == last_step)
    def _():
        scatter_rows((acc_ref,), (rcv_ref,), base, msg_ref, EDGE_BLK, copies, stride)

    @pl.when(step == pl.num_programs(0) - 1)
    def _():
        def fin(it, carry):
            for slot, out in enumerate(slot_views(sa_ref, sb_ref)):
                total = acc_ref[pl.ds(it * (4 * NODE_BLK) + slot, NODE_BLK, stride=4), :]
                for cp in range(1, copies):
                    total = total + acc_ref[pl.ds(it * (4 * NODE_BLK) + slot + cp * stride, NODE_BLK, stride=4), :]
                out[pl.ds(pl.multiple_of(it * NODE_BLK, 8), NODE_BLK), :] = total
            return carry

        lax.fori_loop(0, pad_nodes // NODE_BLK, fin, 0)


def slot_parts(rows, cuts):
    far = [sds((num * EDGE_BLK, LANES), F32) for num in cuts] * 2
    near = [sds((rows, LANES), BF16), sds((rows, LANES), F32)]
    return near + far, [rows_spec(EDGE_BLK, LANES)] * 2 + part_specs(cuts) * 2


def edge_forward(snd, rcv, xs, ps, pr, w1, w2t, vec, cuts, pad_nodes):
    rows, width = len(snd), wide(w1)
    copies = 4
    news, new_specs = slot_parts(rows, cuts) if cuts else ([sds((rows, width), BF16)], [rows_spec(EDGE_BLK, width)])
    saved = [sds((rows, width), F32), sds((rows, width), F32), sds((rows, LANES), F32)]
    sums = [sds((2, pad_nodes, LANES), F32)] * 2
    in_specs = [rows_spec(EDGE_BLK, wide(x)) for x in xs]
    in_specs += [whole_spec(a.shape) for a in (ps, pr, w1, w2t, vec)]
    out_specs = [rows_spec(EDGE_BLK, wide(o)) for o in saved] + new_specs + [whole_spec(o.shape) for o in sums]
    scratch = [pltpu.VMEM((4 * EDGE_BLK, LANES), F32), pltpu.VMEM((4 * EDGE_BLK, LANES), F32),
               pltpu.VMEM((copies * 4 * pad_nodes, LANES), F32), pltpu.VMEM((EDGE_BLK, 2 * LANES), F32)]
    return call(functools.partial(edge_fwd_body, len(xs), cuts, pad_nodes, copies), (rows // EDGE_BLK,), in_specs, out_specs,
                saved + news + sums, scratch, prefetch=2, work=12)(snd, rcv, *xs, ps, pr, w1, w2t, vec)


def edge_bwd_body(n_in, cuts, pad_nodes, copies, snd_ref, rcv_ref, *refs):
    n_g = 2 + 2 * len(cuts) if cuts else 1
    g_refs = refs[:n_g]
    x_refs = refs[n_g:n_g + n_in]
    hid_ref, nrm_ref, inv_ref, ds_ref, w1_ref, w2t_ref, vec_ref = refs[n_g + n_in:n_g + n_in + 7]
    rest = refs[n_g + n_in + 7:]
    n_out = 1 if cuts else 4
    d_refs = rest[:n_out]
    dw1_ref, dw2t_ref, small_ref, ts_ref, tr_ref, gat_ref, dh_ref, accs_ref, accr_ref, sums_ref, far_ref = rest[n_out:]
    step = pl.program_id(0)
    base = step * EDGE_BLK
    stride = 4 * pad_nodes
    last_step = pl.num_programs(0) - 1

    @pl.when(step == 0)
    def _():
        zero_rows(accs_ref, stride * copies, stride // 4)
        zero_rows(accr_ref, stride * copies, stride // 4)
        for ref in (dh_ref, dw1_ref, dw2t_ref, sums_ref):
            ref[ALL] = jnp.zeros(ref.shape, F32)
        gather_rows((ds_ref,), (rcv_ref,), base, gat_ref, EDGE_BLK)

    if cuts:
        lo = 0
        for num, ref2, ref3 in zip(cuts, g_refs[2:], g_refs[2 + len(cuts):]):
            @pl.when(in_part(lo, num))
            def _():
                far_ref[:, :LANES] = ref2[ALL]
                far_ref[:, LANES:] = ref3[ALL]

            lo += num
        g_refs = list(g_refs[:2]) + [far_ref]
    d_edge = jnp.concatenate([ref[ALL].astype(F32) for ref in g_refs], axis=-1)
    d_message = jnp.concatenate(
        [col(d_edge, slot) + gat_ref[pl.ds(slot, EDGE_BLK, stride=4), :] for slot in range(4)], axis=-1)
    scatter_flat((accs_ref, accr_ref), (snd_ref, rcv_ref), jnp.maximum(base - EDGE_BLK, 0), dh_ref, range(EDGE_BLK), copies, stride)
    gather_flat((ds_ref,), (rcv_ref,), jnp.minimum(base + EDGE_BLK, last_step * EDGE_BLK), gat_ref, range(EDGE_BLK))
    d_out_bf, act, d_hidden, sums = mlp_back(
        d_message, hid_ref[ALL], nrm_ref[ALL], inv_ref[:, 0:1], w2t_ref[ALL], vec_ref)
    d_hidden_bf = d_hidden.astype(BF16)
    x_in = jnp.concatenate([ref[ALL].astype(BF16) for ref in x_refs], axis=-1)
    dw2t_ref[ALL] += dot_ta(d_out_bf, act)
    dw1_ref[ALL] += dot_ta(x_in, d_hidden_bf)
    sums_ref[ALL] += jnp.concatenate(sums, axis=0)
    d_x = (d_edge + dot_tb(d_hidden_bf, w1_ref[ALL])).astype(BF16)
    if cuts:
        d_refs[0][ALL] = d_x
    else:
        for slot in range(4):
            d_refs[slot][ALL] = col(d_x, slot).astype(d_refs[slot].dtype)
    for slot in range(4):
        dh_ref[pl.ds(slot, EDGE_BLK, stride=4), :] = col(d_hidden, slot)

    @pl.when(step == last_step)
    def _():
        scatter_rows((accs_ref, accr_ref), (snd_ref, rcv_ref), base, dh_ref, EDGE_BLK, copies, stride)
        total = [jnp.sum(sums_ref[8 * k:8 * k + 8, :], axis=0, keepdims=True) for k in range(4)]
        small_ref[ALL] = jnp.concatenate(total + [jnp.zeros((4, wide(small_ref)), F32)], axis=0)

        def fin(it, carry):
            for acc_ref, out_ref in ((accs_ref, ts_ref), (accr_ref, tr_ref)):
                for slot in range(4):
                    total = acc_ref[pl.ds(it * (4 * NODE_BLK) + slot, NODE_BLK, stride=4), :]
                    for cp in range(1, copies):
                        total = total + acc_ref[pl.ds(it * (4 * NODE_BLK) + slot + cp * stride, NODE_BLK, stride=4), :]
                    out_ref[pl.ds(pl.multiple_of(it * NODE_BLK, 16), NODE_BLK),
                            slot * LANES:(slot + 1) * LANES] = total.astype(BF16)
            return carry

        lax.fori_loop(0, pad_nodes // NODE_BLK, fin, 0)


def edge_backward(snd, rcv, gs, xs, saved, ds, w1, w2t, vec, cuts, pad_nodes):
    rows, width = len(snd), wide(w1)
    copies = 2
    slot_shapes = [sds((rows, LANES), BF16)] + [sds((rows, LANES), F32)] * 3
    d_shapes = [sds((rows, width), BF16)] if cuts else slot_shapes
    tail = [sds((width, width), F32), sds((width, width), F32), sds((8, width), F32),
            sds((pad_nodes, width), BF16), sds((pad_nodes, width), BF16)]
    g_specs = slot_parts(rows, cuts)[-1] if cuts else [rows_spec(EDGE_BLK, width)]
    ins = list(xs) + list(saved)
    in_specs = g_specs + [rows_spec(EDGE_BLK, wide(x)) for x in ins] + [whole_spec(a.shape) for a in (ds, w1, w2t, vec)]
    out_specs = [rows_spec(EDGE_BLK, wide(o)) for o in d_shapes] + [whole_spec(o.shape) for o in tail]
    table = pltpu.VMEM((copies * 4 * pad_nodes, LANES), F32)
    scratch = [pltpu.VMEM((4 * EDGE_BLK, LANES), F32), pltpu.VMEM((4 * EDGE_BLK, LANES), F32), table, table,
               pltpu.VMEM((4 * 8, width), F32), pltpu.VMEM((EDGE_BLK, 2 * LANES), F32)]
    return call(functools.partial(edge_bwd_body, len(xs), cuts, pad_nodes, copies), (rows // EDGE_BLK,), in_specs, out_specs,
                d_shapes + tail, scratch, prefetch=2, work=20)(snd, rcv, *gs, *ins, ds, w1, w2t, vec)


def proj_bwd_body(ts_ref, tr_ref, v_ref, w1s_ref, w1r_ref, dw1e_ref, dw2t_ref, small_ref, node_b1_ref,
                  da_ref, db_ref, ga_ref, gb_ref, acc_s, acc_r):
    step = pl.program_id(0)
    first = step == 0
    d_v = dot_tb(ts_ref[ALL], w1s_ref[ALL]) + dot_tb(tr_ref[ALL], w1r_ref[ALL])
    for slot, out in enumerate(slot_views(da_ref, db_ref)):
        out[ALL] = col(d_v, slot)
    add_to(acc_s, FULL, dot_ta(v_ref[ALL], ts_ref[ALL]), first)
    add_to(acc_r, FULL, dot_ta(v_ref[ALL], tr_ref[ALL]), first)

    @pl.when(step == pl.num_programs(0) - 1)
    def _():
        for slot, out in enumerate(slot_views(ga_ref, gb_ref)):
            rows = slice(slot * LANES, (slot + 1) * LANES)
            for part, src in enumerate((dw1e_ref, acc_s, acc_r, dw2t_ref)):
                out[part * LANES:(part + 1) * LANES, :] = src[rows, :]
            vec_row = jnp.concatenate(
                [small_ref[k:k + 1, rows] for k in range(3)] + [jnp.zeros((1, LANES), F32)], axis=-1)
            out[512:520, :] = jnp.concatenate(
                [vec_row, small_ref[3:4, :], node_b1_ref[0:1, :], jnp.zeros((5, wide(vec_row)), F32)], axis=0)


def proj_backward(ts, tr, v_full, w1s, w1r, dw1e, dw2t, small, node_b1):
    nodes, width = v_full.shape
    ins = [ts, tr, v_full, w1s, w1r, dw1e, dw2t, small, node_b1]
    outs = [sds((2, nodes, LANES), F32)] * 2 + [sds((2, width + 8, width), F32)] * 2
    in_specs = [rows_spec(NODE_BLK, width)] * 3 + [whole_spec(a.shape) for a in ins[3:]]
    out_specs = [pair_spec(NODE_BLK)] * 2 + [whole_spec(outs[2].shape)] * 2
    scratch = [pltpu.VMEM((width, width), F32)] * 2
    return call(proj_bwd_body, (nodes // NODE_BLK,), in_specs, out_specs, outs, scratch)(*ins)


def write_table(ref, val):
    for slot in range(4):
        ref[pl.ds(slot, NODE_BLK, stride=4), :] = col(val, slot)


def node_proj_body(v0_ref, v1_ref, v2_ref, v3_ref, w1s_ref, w1r_ref, b1_ref, v_ref, ps_ref, pr_ref):
    v_in = jnp.concatenate([ref[ALL].astype(BF16) for ref in (v0_ref, v1_ref, v2_ref, v3_ref)], axis=-1)
    v_ref[ALL] = v_in
    write_table(ps_ref, dot(v_in, w1s_ref[ALL]) + b1_ref[0:1, :])
    write_table(pr_ref, dot(v_in, w1r_ref[ALL]))


def node_project(vs, w1s, w1r, b1):
    nodes, width = vs[0].shape[0], w1s.shape[0]
    in_specs = [rows_spec(NODE_BLK, LANES)] * 4 + [whole_spec(a.shape) for a in (w1s, w1r, b1)]
    outs = [sds((nodes, width), BF16), sds((4 * nodes, LANES), F32), sds((4 * nodes, LANES), F32)]
    out_specs = [rows_spec(NODE_BLK, width)] + [rows_spec(4 * NODE_BLK, LANES)] * 2
    return call(node_proj_body, (nodes // NODE_BLK,), in_specs, out_specs, outs, [])(
        *vs, w1s, w1r, b1)


def read_pairs(a_ref, b_ref):
    return jnp.concatenate([a_ref[0], b_ref[0], a_ref[1], b_ref[1]], axis=-1)


def node_fwd_body(v_ref, sa_ref, sb_ref, w1_ref, w2t_ref, vec_ref, b1_ref, w1s_ref, w1r_ref, eb1_ref,
                  new_ref, s_ref, hid_ref, nrm_ref, inv_ref, ps_ref, pr_ref):
    v_in = v_ref[ALL]
    s_in = read_pairs(sa_ref, sb_ref).astype(BF16)
    s_ref[ALL] = s_in
    hidden = dot(v_in, w1_ref[0]) + dot(s_in, w1_ref[1]) + b1_ref[0:1, :]
    hid_ref[ALL] = hidden
    _, normed, inv_std, message = mlp_tail(hidden, w2t_ref[ALL], vec_ref)
    nrm_ref[ALL] = normed
    inv_ref[ALL] = jnp.broadcast_to(inv_std, (NODE_BLK, LANES))
    new = (v_in.astype(F32) + message.astype(F32)).astype(BF16)
    new_ref[ALL] = new
    write_table(ps_ref, dot(new, w1s_ref[ALL]) + eb1_ref[0:1, :])
    write_table(pr_ref, dot(new, w1r_ref[ALL]))


def node_forward(v_in, sa, sb, w1, w2t, vec, b1, w1s, w1r, eb1):
    nodes, width = v_in.shape
    in_specs = [rows_spec(NODE_BLK, width), pair_spec(NODE_BLK), pair_spec(NODE_BLK)]
    in_specs += [whole_spec(a.shape) for a in (w1, w2t, vec, b1, w1s, w1r, eb1)]
    outs = [sds((nodes, width), BF16), sds((nodes, width), BF16), sds((nodes, width), F32), sds((nodes, width), F32),
            sds((nodes, LANES), F32), sds((4 * nodes, LANES), F32), sds((4 * nodes, LANES), F32)]
    out_specs = [rows_spec(NODE_BLK, wide(o)) for o in outs[:5]] + [rows_spec(4 * NODE_BLK, LANES)] * 2
    return call(node_fwd_body, (nodes // NODE_BLK,), in_specs, out_specs, outs, [])(
        v_in, sa, sb, w1, w2t, vec, b1, w1s, w1r, eb1)


def node_grads(first, d_message, v_in, s_in, hidden, normed, inv_std, w1_ref, w2t_ref, vec_ref, ds_ref, gn_ref, db1_ref):
    d_out_bf, act, d_hidden, sums = mlp_back(d_message, hidden, normed, inv_std, w2t_ref[ALL], vec_ref)
    d_hidden_bf = d_hidden.astype(BF16)
    write_table(ds_ref, dot_tb(d_hidden_bf, w1_ref[1]))
    whole = slice(None)
    add_to(gn_ref, (slice(0, LANES), whole), dot_ta(col(v_in, 0), d_hidden_bf), first)
    add_to(gn_ref, (slice(LANES, 2 * LANES), whole), dot_ta(col(s_in, 0), d_hidden_bf), first)
    add_to(gn_ref, (slice(2 * LANES, 3 * LANES), whole), dot_ta(col(d_out_bf, 0), act), first)
    add_to(gn_ref, (slice(3 * LANES, 3 * LANES + 8), whole),
           jnp.concatenate([col(x, 0) for x in sums[:3]] + [jnp.zeros((8, LANES), F32)], axis=-1), first)
    add_to(db1_ref, (whole, whole), sums[3], first)
    return dot_tb(d_hidden_bf, w1_ref[0])


def node_top_body(v_ref, sa_ref, sb_ref, g0_ref, g1_ref, g2_ref, g3_ref, w1_ref, w2t_ref, vec_ref, b1_ref,
                  new_ref, ds_ref, dv_ref, gn_ref, db1_ref):
    first = pl.program_id(0) == 0
    v_in = v_ref[ALL]
    s_in = read_pairs(sa_ref, sb_ref).astype(BF16)
    hidden = dot(v_in, w1_ref[0]) + dot(s_in, w1_ref[1]) + b1_ref[0:1, :]
    _, normed, inv_std, message = mlp_tail(hidden, w2t_ref[ALL], vec_ref)
    new_ref[ALL] = (col(v_in, 0).astype(F32) + col(message, 0).astype(F32)).astype(BF16)
    d_new = jnp.concatenate([ref[ALL].astype(F32) for ref in (g0_ref, g1_ref, g2_ref, g3_ref)], axis=-1)
    dv_ref[ALL] = d_new + node_grads(
        first, d_new, v_in, s_in, hidden, normed, inv_std, w1_ref, w2t_ref, vec_ref, ds_ref, gn_ref, db1_ref)


def node_top(v_in, sa, sb, gs, w1, w2t, vec, b1):
    nodes, width = v_in.shape
    in_specs = [rows_spec(NODE_BLK, width), pair_spec(NODE_BLK), pair_spec(NODE_BLK)] + [rows_spec(NODE_BLK, LANES)] * 4
    in_specs += [whole_spec(a.shape) for a in (w1, w2t, vec, b1)]
    outs = [sds((nodes, LANES), BF16), sds((4 * nodes, LANES), F32), sds((nodes, width), F32),
            sds((3 * LANES + 8, width), F32), sds((8, width), F32)]
    out_specs = [rows_spec(NODE_BLK, LANES), rows_spec(4 * NODE_BLK, LANES), rows_spec(NODE_BLK, width),
                 whole_spec(outs[3].shape), whole_spec(outs[4].shape)]
    return call(node_top_body, (nodes // NODE_BLK,), in_specs, out_specs, outs, [])(
        v_in, sa, sb, *gs, w1, w2t, vec, b1)


def node_bwd_body(dv_ref, ta_ref, tb_ref, v_ref, s_ref, hid_ref, nrm_ref, inv_ref, w1_ref, w2t_ref, vec_ref,
                  ds_ref, dvo_ref, gn_ref, db1_ref):
    first = pl.program_id(0) == 0
    d_new = (dv_ref[ALL] + read_pairs(ta_ref, tb_ref)).astype(BF16).astype(F32)
    d_v = node_grads(first, d_new, v_ref[ALL], s_ref[ALL], hid_ref[ALL], nrm_ref[ALL], inv_ref[:, 0:1],
                     w1_ref, w2t_ref, vec_ref, ds_ref, gn_ref, db1_ref)
    dvo_ref[ALL] = col(d_new, 0) + col(d_v, 0)


def node_backward(dv, ta, tb, v_in, s_in, saved, w1, w2t, vec):
    nodes, width = v_in.shape
    ins = [dv, ta, tb, v_in, s_in, *saved]
    in_specs = [rows_spec(NODE_BLK, width), pair_spec(NODE_BLK), pair_spec(NODE_BLK)]
    in_specs += [rows_spec(NODE_BLK, wide(a)) for a in ins[3:]] + [whole_spec(a.shape) for a in (w1, w2t, vec)]
    outs = [sds((4 * nodes, LANES), F32), sds((nodes, LANES), F32), sds((3 * LANES + 8, width), F32), sds((8, width), F32)]
    out_specs = [rows_spec(4 * NODE_BLK, LANES), rows_spec(NODE_BLK, LANES), whole_spec(outs[2].shape),
                 whole_spec(outs[3].shape)]
    return call(node_bwd_body, (nodes // NODE_BLK,), in_specs, out_specs, outs, [])(
        *ins, w1, w2t, vec)


def part_copies(buf, parts, sem, slot, outward):
    lo, copies = 0, []
    for k, part in enumerate(parts):
        here = buf.at[pl.ds(lo, len(part))]
        src, dst = (here, part) if outward else (part, here)
        copies.append(pltpu.make_async_copy(src, dst, sem.at[slot, k]))
        lo += len(part)
    return copies


def split_slots(refs, num):
    return [refs[:1], refs[1:2], refs[2:2 + num], refs[2 + num:]]


def to_slots_body(limit, num, me_ref, x_ref, *refs):
    slots = split_slots(refs[:-3], num)
    own, far, sem = refs[-3:]
    step = pl.program_id(0)
    rows = len(x_ref)
    row = lax.broadcasted_iota(jnp.int32, x_ref.shape, 0) + (me_ref[0] ^ step) * rows
    val = jnp.where(row < limit, x_ref[ALL].astype(F32), 0.0)
    moves = [part_copies(own if k == 0 else far.at[k - 1], parts, sem, k, True) for k, parts in enumerate(slots)]
    for k, copies in enumerate(moves):
        @pl.when(step == k)
        def _():
            if k == 0:
                own[ALL] = val.astype(BF16)
            else:
                far[k - 1] = val
            for copy in copies:
                copy.start()

    @pl.when(step == len(slots) - 1)
    def _():
        for copies in moves:
            for copy in copies:
                copy.wait()


def slot_buffers(rows, num):
    return [pltpu.VMEM((rows, LANES), BF16), pltpu.VMEM((3, rows, LANES), F32), pltpu.SemaphoreType.DMA((4, num))]


ANYWHERE = pl.BlockSpec(memory_space=pl.ANY)


def to_slots(me, val, rows, cuts):
    outs, _ = slot_parts(rows, cuts)
    return call(functools.partial(to_slots_body, len(val), len(cuts)), (4,),
                [pl.BlockSpec((rows, LANES), lambda d, me: (me[0] ^ d, 0))], [ANYWHERE] * len(outs), outs,
                slot_buffers(rows, len(cuts)), prefetch=1)(me, val)


def from_slots_body(num, me_ref, *refs):
    slots = split_slots(refs[:-4], num)
    out_ref, own, far, sem = refs[-4:]
    step = pl.program_id(0)
    moves = [part_copies(own if k == 0 else far.at[k - 1], parts, sem, k, False) for k, parts in enumerate(slots)]

    @pl.when(step == 0)
    def _():
        for copies in moves:
            for copy in copies:
                copy.start()

    for k, copies in enumerate(moves):
        @pl.when(step == k)
        def _():
            for copy in copies:
                copy.wait()
            out_ref[ALL] = own[ALL] if k == 0 else far[k - 1].astype(BF16)


def from_slots(me, slots, num, limit):
    rows = len(slots[0])
    return call(functools.partial(from_slots_body, num), (4,), [ANYWHERE] * len(slots),
                pl.BlockSpec((rows, LANES), lambda d, me: (me[0] ^ d, 0)), sds((limit, LANES), BF16),
                slot_buffers(rows, num), prefetch=1)(me, *slots)


def unpack_body(per, half_ref, *refs):
    near, far, outs = refs[:2], refs[2:6], refs[6:]
    for k, refs_of in enumerate((near[:1] * 2, near[1:] * 2, far[:2], far[2:])):
        dst = slice(k * LANES, (k + 1) * LANES)
        for p, out in enumerate(outs):
            src = pl.ds(p % per * LANES, LANES)
            if k < 2:
                out[dst, :] = refs_of[0][p // per, src, :].astype(BF16)
                continue
            for mine in range(2):
                @pl.when(half_ref[0] == mine)
                def _():
                    out[dst, :] = refs_of[p // per ^ mine][src, :].astype(BF16)


def unpack_weights(half, slots, per):
    width = wide(slots[0])
    outs = [sds((4 * LANES, width), BF16)] * (2 * per)
    return call(functools.partial(unpack_body, per), (1,), [whole_spec(s.shape) for s in slots],
                [whole_spec(o.shape) for o in outs], outs, [], prefetch=1)(half, *slots)


IN_CUTS = (20,)
GRAD_CUTS = (4, 7, 9)
OUT_CUTS = (12, 8)


class Layer(NamedTuple):
    w1: Any
    ws: Any
    wr: Any
    w2t: Any
    vec: Any
    b1: Any
    node_w1: Any
    node_w2t: Any
    node_vec: Any
    node_b1: Any


def solution(mesh):
    lat_spec = P('dp', None, 'tp')
    first_spec = P(None, None, 'tp', None)
    col_spec = P(None, None, 'tp')
    param_specs = (first_spec, P(), col_spec, col_spec, first_spec, P(), col_spec, col_spec)
    in_specs = (lat_spec, lat_spec, P(), P(), lat_spec, lat_spec) + param_specs
    out_specs = (lat_spec, lat_spec, lat_spec, lat_spec) + param_specs
    tp = mesh.shape['tp']

    def swap(val, mask):
        return lax.ppermute(val, 'tp', [(i, i ^ mask) for i in range(tp)])

    def swap_dp(val):
        return lax.ppermute(val, 'dp', [(0, 1), (1, 0)])

    def local_step(node_lat, edge_lat, senders, receivers, grad_node, grad_edge,
                   edge_w1, edge_b1, edge_w2, edge_vec, node_w1, node_b1, node_w2, node_vec):
        me, half = lax.axis_index('tp'), lax.axis_index('dp')
        _, nodes, _ = node_lat.shape
        _, edges, _ = edge_lat.shape
        width = wide(edge_b1)
        rows = -(-edges // (tp * EDGE_BLK)) * EDGE_BLK
        pad_nodes = (nodes // NODE_BLK + 1) * NODE_BLK
        me_ref, half_ref = me.astype(jnp.int32)[None], half.astype(jnp.int32)[None]

        def to_rows(val, cuts):
            own, near, *far = to_slots(me_ref, val, rows, cuts)
            num = len(cuts)
            moved = [swap(part, 2 + k // num) for k, part in enumerate(far)]
            return [own, swap(near, 1)] + moved

        def to_columns(parts, cuts):
            own, near, *far = parts
            num = len(cuts)
            moved = [swap(part, 2 + k // num) for k, part in enumerate(far)]
            return from_slots(me_ref, [own, swap(near, 1)] + moved, num, edges)[None]

        def my_index(ids):
            padded = jnp.pad(ids, (0, tp * rows - edges), constant_values=nodes)
            return lax.dynamic_slice(padded, (me * rows,), (rows,)) * 4

        def node_slots(val):
            padded = jnp.pad(val, ((0, pad_nodes - nodes), (0, 0)))
            val = padded.astype(F32)
            far = swap(val, 2)
            return [padded, swap(val, 1), far, swap(far, 1)]

        def weight_slots(val):
            far = swap(lax.dynamic_index_in_dim(val, half, 0, keepdims=False), 2)
            rest = swap_dp(far)
            return [val, swap(val, 1), far, rest, swap(far, 1), swap(rest, 1)]

        def pack(l, w1, w2):
            return jnp.concatenate([w1[l].reshape(-1, width), w2[l].T], axis=0).astype(F32)

        vecs = jnp.concatenate([edge_vec.reshape(-1), node_vec.reshape(-1)]).reshape(-1, width)
        vecs = jnp.pad(vecs, ((0, 8 - len(vecs)), (0, 0)))
        group_a = jnp.concatenate([pack(0, edge_w1, edge_w2).reshape(2, -1, width), jnp.stack([vecs, vecs])], axis=1)
        group_b = jnp.concatenate([pack(0, node_w1, node_w2), pack(1, edge_w1, edge_w2), pack(1, node_w1, node_w2)])
        v_slots = node_slots(node_lat[0])
        slots_a = weight_slots(group_a)
        x_slots = to_rows(edge_lat[0], IN_CUTS)
        slots_b = weight_slots(group_b.reshape(2, -1, width))
        g_slots = to_rows(grad_edge[0], GRAD_CUTS)
        gn_slots = node_slots(grad_node[0])
        snd, rcv = my_index(senders), my_index(receivers)

        mats_a = unpack_weights(half_ref, slots_a, 2)
        mats_b = unpack_weights(half_ref, slots_b, 5)
        nv0, ns0, nt0, *edge_mats, nv1, ns1, nt1 = mats_b
        own_a, near_a, far_a, _, cross_a, _ = slots_a
        vec_rows = [s[2 * LANES:2 * LANES + 3].reshape(2, 2, 3, LANES) for s in (own_a[0], near_a[0], far_a, cross_a)]
        (vec0, vec1), (nvec0, nvec1) = jnp.pad(jnp.concatenate(vec_rows, axis=-1), ((0, 0), (0, 0), (0, 5), (0, 0)))
        (eb0, eb1), (nb0, nb1) = [jnp.broadcast_to(b[:, None], (2, 8, width)) for b in (edge_b1, node_b1)]
        low = Layer(*mats_a, vec0, eb0, jnp.stack([nv0, ns0]), nt0, nvec0, nb0)
        top = Layer(*edge_mats, vec1, eb1, jnp.stack([nv1, ns1]), nt1, nvec1, nb1)

        def all_sum(pair_a, pair_b):
            chip = pair_a + swap(pair_b, 1)
            total = chip + swap(chip, 2)[::-1]
            return total, swap(total, 1)

        def own_sum(pair_a, pair_b):
            chip = pair_a + swap(pair_b, 1)
            return chip[0] + swap(chip[1], 2)

        v0, ps, pr = node_project(v_slots, low.ws, low.wr, low.b1)
        hid0, nrm0, inv0, e1, sa, sb = edge_forward(
            snd, rcv, x_slots, ps, pr, low.w1, low.w2t, low.vec, (), pad_nodes)
        sa, sb = all_sum(sa, sb)
        v1, s0, nhid, nnrm, ninv, ps, pr = node_forward(
            v0, sa, sb, low.node_w1, low.node_w2t, low.node_vec, low.node_b1, top.ws, top.wr, top.b1)
        hid1, nrm1, inv1, *parts, sa, sb = edge_forward(
            snd, rcv, [e1], ps, pr, top.w1, top.w2t, top.vec, OUT_CUTS, pad_nodes)
        edge_out = to_columns(parts, OUT_CUTS)
        sa, sb = all_sum(sa, sb)

        v2, ds, dv, gn1, ndb1 = node_top(
            v1, sa, sb, gn_slots, top.node_w1, top.node_w2t, top.node_vec, top.node_b1)
        node_out = v2[:nodes][None]

        def mine_only(db1):
            lane = lax.broadcasted_iota(jnp.int32, db1.shape, 1)
            return jnp.broadcast_to(jnp.where(lane // LANES == me, db1, 0.0).sum(axis=0), db1.shape)

        d_e1, dw1e, dw2t, small, ts, tr = edge_backward(
            snd, rcv, g_slots, [e1], (hid1, nrm1, inv1), ds, top.w1, top.w2t, top.vec,
            GRAD_CUTS, pad_nodes)
        da, db, *ge1 = proj_backward(ts, tr, v1, top.ws, top.wr, dw1e, dw2t, small, mine_only(ndb1))
        da, db = all_sum(da, db)
        ds, dv_own, gn0, ndb1 = node_backward(
            dv, da, db, v0, s0, (nhid, nnrm, ninv), low.node_w1, low.node_w2t, low.node_vec)
        *d_slots, dw1e, dw2t, small, ts, tr = edge_backward(
            snd, rcv, [d_e1], x_slots, (hid0, nrm0, inv0), ds, low.w1, low.w2t, low.vec,
            (), pad_nodes)
        d_edge = to_columns(d_slots, IN_CUTS)
        da, db, *ge0 = proj_backward(ts, tr, v0, low.ws, low.wr, dw1e, dw2t, small, mine_only(ndb1))
        d_node = (dv_own + own_sum(da, db))[:nodes].astype(BF16)[None]

        ge = [own_sum(*ge0), own_sum(*ge1)]
        ge = [g + swap_dp(g) for g in ge]
        gn = [g + swap_dp(g) for g in (gn0, gn1)]
        stack = lambda fn: jnp.stack([fn(l) for l in range(2)])
        w1_rows, w2_rows, vec_wide = 3 * LANES, 4 * LANES, 3 * LANES
        return (node_out, edge_out, d_node, d_edge,
                stack(lambda l: ge[l][:w1_rows].reshape(3, LANES, width)),
                stack(lambda l: ge[l][w2_rows + 1]),
                stack(lambda l: ge[l][w1_rows:w2_rows].T),
                stack(lambda l: ge[l][w2_rows, :vec_wide].reshape(3, LANES)),
                stack(lambda l: gn[l][:2 * LANES].reshape(2, LANES, width)),
                stack(lambda l: ge[l][w2_rows + 2]),
                stack(lambda l: gn[l][2 * LANES:w1_rows].T),
                stack(lambda l: gn[l][w1_rows:, :vec_wide].sum(axis=0).reshape(3, LANES)))

    return jax.shard_map(local_step, mesh=mesh, in_specs=in_specs, out_specs=out_specs, check_vma=False)
```

```python
import functools
from typing import Any, NamedTuple

import jax
import jax.numpy as jnp
from jax import lax
from jax.experimental import pallas as pl
from jax.experimental.pallas import tpu as pltpu
from jax.sharding import PartitionSpec as P


LN_EPS = 1e-5
F32 = jnp.float32
BF16 = jnp.bfloat16
LANES = 128
EDGE_BLK = 256
NODE_BLK = 368
GATHER_UNROLL = 16
ALL = Ellipsis
FULL = (slice(None), slice(None))
VMEM_BYTES = 64 * 2**20 - 2**16


WORK = 4 * 10**9


def wide(val):
    return val.shape[-1]


def slot_views(pair_a, pair_b):
    return pair_a.at[0], pair_b.at[0], pair_a.at[1], pair_b.at[1]


def dot(lhs, rhs):
    return lax.dot_general(lhs, rhs, (((1,), (0,)), ((), ())), preferred_element_type=F32)


def dot_tb(lhs, rhs):
    return lax.dot_general(lhs, rhs, (((1,), (1,)), ((), ())), preferred_element_type=F32)


def dot_ta(lhs, rhs):
    return lax.dot_general(lhs, rhs, (((0,), (0,)), ((), ())), preferred_element_type=F32)


def col(val, slot):
    return val[:, slot * LANES:(slot + 1) * LANES]


def gather_rows(tables, index_refs, base, out_ref, num_rows):
    def step(it, carry):
        for sub in range(GATHER_UNROLL):
            row = it * GATHER_UNROLL + sub
            acc = None
            for table, index_ref in zip(tables, index_refs):
                val = table[pl.ds(pl.multiple_of(index_ref[base + row], 4), 4), :]
                acc = val if acc is None else acc + val
            out_ref[pl.ds(pl.multiple_of(row * 4, 4), 4), :] = acc
        return carry

    lax.fori_loop(0, num_rows // GATHER_UNROLL, step, 0)


def scatter_rows(accs, index_refs, base, src_ref, num_rows, copies, stride):
    def step(it, carry):
        pending = []
        for sub in range(copies):
            row = it * copies + sub
            val = src_ref[pl.ds(pl.multiple_of(row * 4, 4), 4), :]
            for acc, index_ref in zip(accs, index_refs):
                at = pl.multiple_of(index_ref[base + row] + sub * stride, 4)
                pending.append((acc, at, acc[pl.ds(at, 4), :] + val))
        for acc, at, val in pending:
            acc[pl.ds(at, 4), :] = val
        return carry

    lax.fori_loop(0, num_rows // copies, step, 0)


def gather_flat(tables, index_refs, base, out_ref, rows):
    for row in rows:
        acc = None
        for table, index_ref in zip(tables, index_refs):
            val = table[pl.ds(pl.multiple_of(index_ref[base + row], 4), 4), :]
            acc = val if acc is None else acc + val
        out_ref[4 * row:4 * row + 4, :] = acc


def scatter_flat(accs, index_refs, base, src_ref, rows, copies, stride):
    for row in rows[::copies]:
        pending = []
        for sub in range(copies):
            val = src_ref[4 * (row + sub):4 * (row + sub) + 4, :]
            for acc, index_ref in zip(accs, index_refs):
                at = pl.multiple_of(index_ref[base + row + sub] + sub * stride, 4)
                pending.append((acc, at, acc[pl.ds(at, 4), :] + val))
        for acc, at, val in pending:
            acc[pl.ds(at, 4), :] = val


def zero_rows(ref, rows, step_rows):
    def step(it, carry):
        ref[pl.ds(pl.multiple_of(it * step_rows, 8), step_rows), :] = jnp.zeros((step_rows, LANES), F32)
        return carry

    lax.fori_loop(0, rows // step_rows, step, 0)


def row_mean(val):
    return jnp.sum(val, axis=-1, keepdims=True) * (1.0 / val.shape[-1])


def mlp_tail(hidden, w2t, vec_ref):
    act = (hidden * jax.nn.sigmoid(hidden)).astype(BF16)
    out = dot_tb(act, w2t) + vec_ref[0:1, :]
    centered = out - row_mean(out)
    inv_std = lax.rsqrt(row_mean(centered * centered) + LN_EPS)
    normed = centered * inv_std
    message = (normed * vec_ref[1:2, :] + vec_ref[2:3, :]).astype(BF16)
    return act, normed, inv_std, message


def mlp_back(d_message, hidden, normed, inv_std, w2t, vec_ref):
    d_normed = d_message * vec_ref[1:2, :]
    d_out = inv_std * (d_normed - row_mean(d_normed) - normed * row_mean(d_normed * normed))
    d_out_bf = d_out.astype(BF16)
    sig = jax.nn.sigmoid(hidden)
    act = (hidden * sig).astype(BF16)
    d_act = dot(d_out_bf, w2t)
    d_hidden = d_act * (sig * (1.0 + hidden * (1.0 - sig)))
    sums = [jnp.sum(x.reshape(-1, 8, wide(x)), axis=0) for x in (d_out, d_message * normed, d_message, d_hidden)]
    return d_out_bf, act, d_hidden, sums


def add_to(ref, idx, val, first):
    @pl.when(first)
    def _():
        ref[idx] = val

    @pl.when(jnp.logical_not(first))
    def _():
        ref[idx] += val


def call(body, grid, in_specs, out_specs, out_shape, scratch, prefetch=0, work=1):
    return pl.pallas_call(
        body,
        out_shape=out_shape,
        grid_spec=pltpu.PrefetchScalarGridSpec(
            num_scalar_prefetch=prefetch, grid=grid, in_specs=in_specs, out_specs=out_specs, scratch_shapes=scratch),
        compiler_params=pltpu.CompilerParams(vmem_limit_bytes=VMEM_BYTES, dimension_semantics=("arbitrary",) * len(grid)),
        cost_estimate=pl.CostEstimate(flops=work * WORK, bytes_accessed=work * WORK // 1000, transcendentals=0))


def rows_spec(blk, width):
    return pl.BlockSpec((blk, width), lambda i, *_: (i, 0))


def whole_spec(shape):
    zeros = (0,) * len(shape)
    return pl.BlockSpec(shape, lambda i, *_: zeros, pipeline_mode=pl.Buffered(1))


def pair_spec(blk):
    return pl.BlockSpec((2, blk, LANES), lambda i, *_: (0, i, 0))


def in_part(lo, num):
    step = pl.program_id(0)
    return jnp.logical_and(step >= lo, step < lo + num)


def part_specs(cuts):
    lows = [sum(cuts[:k]) for k in range(len(cuts))]
    return [pl.BlockSpec((EDGE_BLK, LANES), lambda i, *_, lo=lo, num=num: (jnp.clip(i - lo, 0, num - 1), 0))
            for lo, num in zip(lows, cuts)]


def sds(shape, dtype):
    return jax.ShapeDtypeStruct(shape, dtype)


def edge_fwd_body(n_in, cuts, pad_nodes, copies, snd_ref, rcv_ref, *refs):
    x_refs = refs[:n_in]
    ps_ref, pr_ref, w1_ref, w2t_ref, vec_ref, hid_ref, nrm_ref, inv_ref = refs[n_in:n_in + 8]
    n_out = 2 + 2 * len(cuts) if cuts else 1
    new_refs = refs[n_in + 8:n_in + 8 + n_out]
    sa_ref, sb_ref, gat_ref, msg_ref, acc_ref, far_ref = refs[n_in + 8 + n_out:]
    step = pl.program_id(0)
    base = step * EDGE_BLK
    stride = 4 * pad_nodes

    last_step = pl.num_programs(0) - 1

    @pl.when(step == 0)
    def _():
        zero_rows(acc_ref, stride * copies, stride // 4)
        msg_ref[ALL] = jnp.zeros(msg_ref.shape, F32)
        gather_rows((ps_ref, pr_ref), (snd_ref, rcv_ref), base, gat_ref, EDGE_BLK)

    x_in = jnp.concatenate([ref[ALL].astype(BF16) for ref in x_refs], axis=-1)
    part = dot(x_in, w1_ref[ALL])
    hidden = jnp.concatenate(
        [col(part, slot) + gat_ref[pl.ds(slot, EDGE_BLK, stride=4), :] for slot in range(4)], axis=-1)
    hid_ref[ALL] = hidden
    scatter_flat((acc_ref,), (rcv_ref,), jnp.maximum(base - EDGE_BLK, 0), msg_ref, range(EDGE_BLK), copies, stride)
    gather_flat((ps_ref, pr_ref), (snd_ref, rcv_ref), jnp.minimum(base + EDGE_BLK, last_step * EDGE_BLK), gat_ref, range(EDGE_BLK))
    _, normed, inv_std, message = mlp_tail(hidden, w2t_ref[ALL], vec_ref)
    nrm_ref[ALL] = normed
    inv_ref[ALL] = jnp.broadcast_to(inv_std, (EDGE_BLK, LANES))
    msg = message.astype(F32)
    new = (x_in.astype(F32) + msg).astype(BF16)
    if cuts:
        new_refs[0][ALL] = col(new, 0)
        new_refs[1][ALL] = col(new, 1).astype(F32)
        far_ref[ALL] = new[:, 2 * LANES:].astype(F32)
        lo = 0
        for num, ref2, ref3 in zip(cuts, new_refs[2:], new_refs[2 + len(cuts):]):
            @pl.when(in_part(lo, num))
            def _():
                ref2[ALL] = col(far_ref, 0)
                ref3[ALL] = col(far_ref, 1)

            lo += num
    else:
        new_refs[0][ALL] = new
    for slot in range(4):
        msg_ref[pl.ds(slot, EDGE_BLK, stride=4), :] = col(msg, slot)

    @pl.when(step == last_step)
    def _():
        scatter_rows((acc_ref,), (rcv_ref,), base, msg_ref, EDGE_BLK, copies, stride)

    @pl.when(step == pl.num_programs(0) - 1)
    def _():
        def fin(it, carry):
            for slot, out in enumerate(slot_views(sa_ref, sb_ref)):
                total = acc_ref[pl.ds(it * (4 * NODE_BLK) + slot, NODE_BLK, stride=4), :]
                for cp in range(1, copies):
                    total = total + acc_ref[pl.ds(it * (4 * NODE_BLK) + slot + cp * stride, NODE_BLK, stride=4), :]
                out[pl.ds(pl.multiple_of(it * NODE_BLK, 8), NODE_BLK), :] = total
            return carry

        lax.fori_loop(0, pad_nodes // NODE_BLK, fin, 0)


def slot_parts(rows, cuts):
    far = [sds((num * EDGE_BLK, LANES), F32) for num in cuts] * 2
    near = [sds((rows, LANES), BF16), sds((rows, LANES), F32)]
    return near + far, [rows_spec(EDGE_BLK, LANES)] * 2 + part_specs(cuts) * 2


def edge_forward(snd, rcv, xs, ps, pr, w1, w2t, vec, cuts, pad_nodes):
    rows, width = len(snd), wide(w1)
    copies = 4
    news, new_specs = slot_parts(rows, cuts) if cuts else ([sds((rows, width), BF16)], [rows_spec(EDGE_BLK, width)])
    saved = [sds((rows, width), F32), sds((rows, width), F32), sds((rows, LANES), F32)]
    sums = [sds((2, pad_nodes, LANES), F32)] * 2
    in_specs = [rows_spec(EDGE_BLK, wide(x)) for x in xs]
    in_specs += [whole_spec(a.shape) for a in (ps, pr, w1, w2t, vec)]
    out_specs = [rows_spec(EDGE_BLK, wide(o)) for o in saved] + new_specs + [whole_spec(o.shape) for o in sums]
    scratch = [pltpu.VMEM((4 * EDGE_BLK, LANES), F32), pltpu.VMEM((4 * EDGE_BLK, LANES), F32),
               pltpu.VMEM((copies * 4 * pad_nodes, LANES), F32), pltpu.VMEM((EDGE_BLK, 2 * LANES), F32)]
    return call(functools.partial(edge_fwd_body, len(xs), cuts, pad_nodes, copies), (rows // EDGE_BLK,), in_specs, out_specs,
                saved + news + sums, scratch, prefetch=2, work=12)(snd, rcv, *xs, ps, pr, w1, w2t, vec)


def edge_bwd_body(n_in, cuts, pad_nodes, copies, snd_ref, rcv_ref, *refs):
    n_g = 2 + 2 * len(cuts) if cuts else 1
    g_refs = refs[:n_g]
    x_refs = refs[n_g:n_g + n_in]
    hid_ref, nrm_ref, inv_ref, ds_ref, w1_ref, w2t_ref, vec_ref = refs[n_g + n_in:n_g + n_in + 7]
    rest = refs[n_g + n_in + 7:]
    n_out = 1 if cuts else 4
    d_refs = rest[:n_out]
    dw1_ref, dw2t_ref, small_ref, ts_ref, tr_ref, gat_ref, dh_ref, accs_ref, accr_ref, sums_ref, far_ref = rest[n_out:]
    step = pl.program_id(0)
    base = step * EDGE_BLK
    stride = 4 * pad_nodes
    last_step = pl.num_programs(0) - 1

    @pl.when(step == 0)
    def _():
        zero_rows(accs_ref, stride * copies, stride // 4)
        zero_rows(accr_ref, stride * copies, stride // 4)
        for ref in (dh_ref, dw1_ref, dw2t_ref, sums_ref):
            ref[ALL] = jnp.zeros(ref.shape, F32)
        gather_rows((ds_ref,), (rcv_ref,), base, gat_ref, EDGE_BLK)

    if cuts:
        lo = 0
        for num, ref2, ref3 in zip(cuts, g_refs[2:], g_refs[2 + len(cuts):]):
            @pl.when(in_part(lo, num))
            def _():
                far_ref[:, :LANES] = ref2[ALL]
                far_ref[:, LANES:] = ref3[ALL]

            lo += num
        g_refs = list(g_refs[:2]) + [far_ref]
    d_edge = jnp.concatenate([ref[ALL].astype(F32) for ref in g_refs], axis=-1)
    d_message = jnp.concatenate(
        [col(d_edge, slot) + gat_ref[pl.ds(slot, EDGE_BLK, stride=4), :] for slot in range(4)], axis=-1)
    scatter_flat((accs_ref, accr_ref), (snd_ref, rcv_ref), jnp.maximum(base - EDGE_BLK, 0), dh_ref, range(EDGE_BLK), copies, stride)
    gather_flat((ds_ref,), (rcv_ref,), jnp.minimum(base + EDGE_BLK, last_step * EDGE_BLK), gat_ref, range(EDGE_BLK))
    d_out_bf, act, d_hidden, sums = mlp_back(
        d_message, hid_ref[ALL], nrm_ref[ALL], inv_ref[:, 0:1], w2t_ref[ALL], vec_ref)
    d_hidden_bf = d_hidden.astype(BF16)
    x_in = jnp.concatenate([ref[ALL].astype(BF16) for ref in x_refs], axis=-1)
    dw2t_ref[ALL] += dot_ta(d_out_bf, act)
    dw1_ref[ALL] += dot_ta(x_in, d_hidden_bf)
    sums_ref[ALL] += jnp.concatenate(sums, axis=0)
    d_x = (d_edge + dot_tb(d_hidden_bf, w1_ref[ALL])).astype(BF16)
    if cuts:
        d_refs[0][ALL] = d_x
    else:
        for slot in range(4):
            d_refs[slot][ALL] = col(d_x, slot).astype(d_refs[slot].dtype)
    for slot in range(4):
        dh_ref[pl.ds(slot, EDGE_BLK, stride=4), :] = col(d_hidden, slot)

    @pl.when(step == last_step)
    def _():
        scatter_rows((accs_ref, accr_ref), (snd_ref, rcv_ref), base, dh_ref, EDGE_BLK, copies, stride)
        total = [jnp.sum(sums_ref[8 * k:8 * k + 8, :], axis=0, keepdims=True) for k in range(4)]
        small_ref[ALL] = jnp.concatenate(total + [jnp.zeros((4, wide(small_ref)), F32)], axis=0)

        def fin(it, carry):
            for acc_ref, out_ref in ((accs_ref, ts_ref), (accr_ref, tr_ref)):
                for slot in range(4):
                    total = acc_ref[pl.ds(it * (4 * NODE_BLK) + slot, NODE_BLK, stride=4), :]
                    for cp in range(1, copies):
                        total = total + acc_ref[pl.ds(it * (4 * NODE_BLK) + slot + cp * stride, NODE_BLK, stride=4), :]
                    out_ref[pl.ds(pl.multiple_of(it * NODE_BLK, 16), NODE_BLK),
                            slot * LANES:(slot + 1) * LANES] = total.astype(BF16)
            return carry

        lax.fori_loop(0, pad_nodes // NODE_BLK, fin, 0)


def edge_backward(snd, rcv, gs, xs, saved, ds, w1, w2t, vec, cuts, pad_nodes):
    rows, width = len(snd), wide(w1)
    copies = 2
    slot_shapes = [sds((rows, LANES), BF16)] + [sds((rows, LANES), F32)] * 3
    d_shapes = [sds((rows, width), BF16)] if cuts else slot_shapes
    tail = [sds((width, width), F32), sds((width, width), F32), sds((8, width), F32),
            sds((pad_nodes, width), BF16), sds((pad_nodes, width), BF16)]
    g_specs = slot_parts(rows, cuts)[-1] if cuts else [rows_spec(EDGE_BLK, width)]
    ins = list(xs) + list(saved)
    in_specs = g_specs + [rows_spec(EDGE_BLK, wide(x)) for x in ins] + [whole_spec(a.shape) for a in (ds, w1, w2t, vec)]
    out_specs = [rows_spec(EDGE_BLK, wide(o)) for o in d_shapes] + [whole_spec(o.shape) for o in tail]
    table = pltpu.VMEM((copies * 4 * pad_nodes, LANES), F32)
    scratch = [pltpu.VMEM((4 * EDGE_BLK, LANES), F32), pltpu.VMEM((4 * EDGE_BLK, LANES), F32), table, table,
               pltpu.VMEM((4 * 8, width), F32), pltpu.VMEM((EDGE_BLK, 2 * LANES), F32)]
    return call(functools.partial(edge_bwd_body, len(xs), cuts, pad_nodes, copies), (rows // EDGE_BLK,), in_specs, out_specs,
                d_shapes + tail, scratch, prefetch=2, work=20)(snd, rcv, *gs, *ins, ds, w1, w2t, vec)


def proj_bwd_body(ts_ref, tr_ref, v_ref, w1s_ref, w1r_ref, dw1e_ref, dw2t_ref, small_ref, node_b1_ref,
                  da_ref, db_ref, ga_ref, gb_ref, acc_s, acc_r):
    step = pl.program_id(0)
    first = step == 0
    d_v = dot_tb(ts_ref[ALL], w1s_ref[ALL]) + dot_tb(tr_ref[ALL], w1r_ref[ALL])
    for slot, out in enumerate(slot_views(da_ref, db_ref)):
        out[ALL] = col(d_v, slot)
    add_to(acc_s, FULL, dot_ta(v_ref[ALL], ts_ref[ALL]), first)
    add_to(acc_r, FULL, dot_ta(v_ref[ALL], tr_ref[ALL]), first)

    @pl.when(step == pl.num_programs(0) - 1)
    def _():
        for slot, out in enumerate(slot_views(ga_ref, gb_ref)):
            rows = slice(slot * LANES, (slot + 1) * LANES)
            for part, src in enumerate((dw1e_ref, acc_s, acc_r, dw2t_ref)):
                out[part * LANES:(part + 1) * LANES, :] = src[rows, :]
            vec_row = jnp.concatenate(
                [small_ref[k:k + 1, rows] for k in range(3)] + [jnp.zeros((1, LANES), F32)], axis=-1)
            out[4 * LANES:, :] = jnp.concatenate(
                [vec_row, small_ref[3:4, :], node_b1_ref[0:1, :], jnp.zeros((13, wide(vec_row)), F32)], axis=0)


def proj_backward(ts, tr, v_full, w1s, w1r, dw1e, dw2t, small, node_b1):
    nodes, width = v_full.shape
    ins = [ts, tr, v_full, w1s, w1r, dw1e, dw2t, small, node_b1]
    outs = [sds((2, nodes, LANES), F32)] * 2 + [sds((2, width + 16, width), F32)] * 2
    in_specs = [rows_spec(NODE_BLK, width)] * 3 + [whole_spec(a.shape) for a in ins[3:]]
    out_specs = [pair_spec(NODE_BLK)] * 2 + [whole_spec(outs[2].shape)] * 2
    scratch = [pltpu.VMEM((width, width), F32)] * 2
    return call(proj_bwd_body, (nodes // NODE_BLK,), in_specs, out_specs, outs, scratch)(*ins)


def write_table(ref, val):
    for slot in range(4):
        ref[pl.ds(slot, NODE_BLK, stride=4), :] = col(val, slot)


def node_proj_body(v0_ref, v1_ref, v2_ref, v3_ref, w1s_ref, w1r_ref, b1_ref, v_ref, ps_ref, pr_ref):
    v_in = jnp.concatenate([ref[ALL].astype(BF16) for ref in (v0_ref, v1_ref, v2_ref, v3_ref)], axis=-1)
    v_ref[ALL] = v_in
    write_table(ps_ref, dot(v_in, w1s_ref[ALL]) + b1_ref[0:1, :])
    write_table(pr_ref, dot(v_in, w1r_ref[ALL]))


def node_project(vs, w1s, w1r, b1):
    nodes, width = vs[0].shape[0], w1s.shape[0]
    in_specs = [rows_spec(NODE_BLK, LANES)] * 4 + [whole_spec(a.shape) for a in (w1s, w1r, b1)]
    outs = [sds((nodes, width), BF16), sds((4 * nodes, LANES), F32), sds((4 * nodes, LANES), F32)]
    out_specs = [rows_spec(NODE_BLK, width)] + [rows_spec(4 * NODE_BLK, LANES)] * 2
    return call(node_proj_body, (nodes // NODE_BLK,), in_specs, out_specs, outs, [])(
        *vs, w1s, w1r, b1)


def read_pairs(a_ref, b_ref):
    return jnp.concatenate([a_ref[0], b_ref[0], a_ref[1], b_ref[1]], axis=-1)


def node_fwd_body(v_ref, sa_ref, sb_ref, w1_ref, w2t_ref, vec_ref, b1_ref, w1s_ref, w1r_ref, eb1_ref,
                  new_ref, s_ref, hid_ref, nrm_ref, inv_ref, ps_ref, pr_ref):
    v_in = v_ref[ALL]
    s_in = read_pairs(sa_ref, sb_ref).astype(BF16)
    s_ref[ALL] = s_in
    hidden = dot(v_in, w1_ref[0]) + dot(s_in, w1_ref[1]) + b1_ref[0:1, :]
    hid_ref[ALL] = hidden
    _, normed, inv_std, message = mlp_tail(hidden, w2t_ref[ALL], vec_ref)
    nrm_ref[ALL] = normed
    inv_ref[ALL] = jnp.broadcast_to(inv_std, (NODE_BLK, LANES))
    new = (v_in.astype(F32) + message.astype(F32)).astype(BF16)
    new_ref[ALL] = new
    write_table(ps_ref, dot(new, w1s_ref[ALL]) + eb1_ref[0:1, :])
    write_table(pr_ref, dot(new, w1r_ref[ALL]))


def node_forward(v_in, sa, sb, w1, w2t, vec, b1, w1s, w1r, eb1):
    nodes, width = v_in.shape
    in_specs = [rows_spec(NODE_BLK, width), pair_spec(NODE_BLK), pair_spec(NODE_BLK)]
    in_specs += [whole_spec(a.shape) for a in (w1, w2t, vec, b1, w1s, w1r, eb1)]
    outs = [sds((nodes, width), BF16), sds((nodes, width), BF16), sds((nodes, width), F32), sds((nodes, width), F32),
            sds((nodes, LANES), F32), sds((4 * nodes, LANES), F32), sds((4 * nodes, LANES), F32)]
    out_specs = [rows_spec(NODE_BLK, wide(o)) for o in outs[:5]] + [rows_spec(4 * NODE_BLK, LANES)] * 2
    return call(node_fwd_body, (nodes // NODE_BLK,), in_specs, out_specs, outs, [])(
        v_in, sa, sb, w1, w2t, vec, b1, w1s, w1r, eb1)


def node_grads(first, d_message, v_in, s_in, hidden, normed, inv_std, w1_ref, w2t_ref, vec_ref, ds_ref, gn_ref, db1_ref):
    d_out_bf, act, d_hidden, sums = mlp_back(d_message, hidden, normed, inv_std, w2t_ref[ALL], vec_ref)
    d_hidden_bf = d_hidden.astype(BF16)
    write_table(ds_ref, dot_tb(d_hidden_bf, w1_ref[1]))
    whole = slice(None)
    add_to(gn_ref, (slice(0, LANES), whole), dot_ta(col(v_in, 0), d_hidden_bf), first)
    add_to(gn_ref, (slice(LANES, 2 * LANES), whole), dot_ta(col(s_in, 0), d_hidden_bf), first)
    add_to(gn_ref, (slice(2 * LANES, 3 * LANES), whole), dot_ta(col(d_out_bf, 0), act), first)
    add_to(gn_ref, (slice(3 * LANES, 3 * LANES + 8), whole),
           jnp.concatenate([col(x, 0) for x in sums[:3]] + [jnp.zeros((8, LANES), F32)], axis=-1), first)
    add_to(db1_ref, (whole, whole), sums[3], first)
    return dot_tb(d_hidden_bf, w1_ref[0])


def node_top_body(v_ref, sa_ref, sb_ref, g0_ref, g1_ref, g2_ref, g3_ref, w1_ref, w2t_ref, vec_ref, b1_ref,
                  new_ref, ds_ref, dv_ref, gn_ref, db1_ref):
    first = pl.program_id(0) == 0
    v_in = v_ref[ALL]
    s_in = read_pairs(sa_ref, sb_ref).astype(BF16)
    hidden = dot(v_in, w1_ref[0]) + dot(s_in, w1_ref[1]) + b1_ref[0:1, :]
    _, normed, inv_std, message = mlp_tail(hidden, w2t_ref[ALL], vec_ref)
    new_ref[ALL] = (col(v_in, 0).astype(F32) + col(message, 0).astype(F32)).astype(BF16)
    d_new = jnp.concatenate([ref[ALL].astype(F32) for ref in (g0_ref, g1_ref, g2_ref, g3_ref)], axis=-1)
    dv_ref[ALL] = d_new + node_grads(
        first, d_new, v_in, s_in, hidden, normed, inv_std, w1_ref, w2t_ref, vec_ref, ds_ref, gn_ref, db1_ref)


def node_top(v_in, sa, sb, gs, w1, w2t, vec, b1):
    nodes, width = v_in.shape
    in_specs = [rows_spec(NODE_BLK, width), pair_spec(NODE_BLK), pair_spec(NODE_BLK)] + [rows_spec(NODE_BLK, LANES)] * 4
    in_specs += [whole_spec(a.shape) for a in (w1, w2t, vec, b1)]
    outs = [sds((nodes, LANES), BF16), sds((4 * nodes, LANES), F32), sds((nodes, width), F32),
            sds((3 * LANES + 8, width), F32), sds((8, width), F32)]
    out_specs = [rows_spec(NODE_BLK, LANES), rows_spec(4 * NODE_BLK, LANES), rows_spec(NODE_BLK, width),
                 whole_spec(outs[3].shape), whole_spec(outs[4].shape)]
    return call(node_top_body, (nodes // NODE_BLK,), in_specs, out_specs, outs, [])(
        v_in, sa, sb, *gs, w1, w2t, vec, b1)


def node_bwd_body(dv_ref, ta_ref, tb_ref, v_ref, s_ref, hid_ref, nrm_ref, inv_ref, w1_ref, w2t_ref, vec_ref,
                  ds_ref, dvo_ref, gn_ref, db1_ref):
    first = pl.program_id(0) == 0
    d_new = (dv_ref[ALL] + read_pairs(ta_ref, tb_ref)).astype(BF16).astype(F32)
    d_v = node_grads(first, d_new, v_ref[ALL], s_ref[ALL], hid_ref[ALL], nrm_ref[ALL], inv_ref[:, 0:1],
                     w1_ref, w2t_ref, vec_ref, ds_ref, gn_ref, db1_ref)
    dvo_ref[ALL] = col(d_new, 0) + col(d_v, 0)


def node_backward(dv, ta, tb, v_in, s_in, saved, w1, w2t, vec):
    nodes, width = v_in.shape
    ins = [dv, ta, tb, v_in, s_in, *saved]
    in_specs = [rows_spec(NODE_BLK, width), pair_spec(NODE_BLK), pair_spec(NODE_BLK)]
    in_specs += [rows_spec(NODE_BLK, wide(a)) for a in ins[3:]] + [whole_spec(a.shape) for a in (w1, w2t, vec)]
    outs = [sds((4 * nodes, LANES), F32), sds((nodes, LANES), F32), sds((3 * LANES + 8, width), F32), sds((8, width), F32)]
    out_specs = [rows_spec(4 * NODE_BLK, LANES), rows_spec(NODE_BLK, LANES), whole_spec(outs[2].shape),
                 whole_spec(outs[3].shape)]
    return call(node_bwd_body, (nodes // NODE_BLK,), in_specs, out_specs, outs, [])(
        *ins, w1, w2t, vec)


def part_copies(buf, parts, sem, slot, outward):
    lo, copies = 0, []
    for k, part in enumerate(parts):
        here = buf.at[pl.ds(lo, len(part))]
        src, dst = (here, part) if outward else (part, here)
        copies.append(pltpu.make_async_copy(src, dst, sem.at[slot, k]))
        lo += len(part)
    return copies


def split_slots(refs, num):
    return [refs[:1], refs[1:2], refs[2:2 + num], refs[2 + num:]]


def to_slots_body(limit, num, me_ref, x_ref, *refs):
    slots = split_slots(refs[:-3], num)
    own, far, sem = refs[-3:]
    step = pl.program_id(0)
    rows = len(x_ref)
    row = lax.broadcasted_iota(jnp.int32, x_ref.shape, 0) + (me_ref[0] ^ step) * rows
    val = jnp.where(row < limit, x_ref[ALL].astype(F32), 0.0)
    moves = [part_copies(own if k == 0 else far.at[k - 1], parts, sem, k, True) for k, parts in enumerate(slots)]
    for k, copies in enumerate(moves):
        @pl.when(step == k)
        def _():
            if k == 0:
                own[ALL] = val.astype(BF16)
            else:
                far[k - 1] = val
            for copy in copies:
                copy.start()

    @pl.when(step == len(slots) - 1)
    def _():
        for copies in moves:
            for copy in copies:
                copy.wait()


def slot_buffers(rows, num):
    return [pltpu.VMEM((rows, LANES), BF16), pltpu.VMEM((3, rows, LANES), F32), pltpu.SemaphoreType.DMA((4, num))]


ANYWHERE = pl.BlockSpec(memory_space=pl.ANY)


def to_slots(me, val, rows, cuts):
    outs, _ = slot_parts(rows, cuts)
    return call(functools.partial(to_slots_body, len(val), len(cuts)), (4,),
                [pl.BlockSpec((rows, LANES), lambda d, me: (me[0] ^ d, 0))], [ANYWHERE] * len(outs), outs,
                slot_buffers(rows, len(cuts)), prefetch=1)(me, val)


def from_slots_body(num, me_ref, *refs):
    slots = split_slots(refs[:-4], num)
    out_ref, own, far, sem = refs[-4:]
    step = pl.program_id(0)
    moves = [part_copies(own if k == 0 else far.at[k - 1], parts, sem, k, False) for k, parts in enumerate(slots)]

    @pl.when(step == 0)
    def _():
        for copies in moves:
            for copy in copies:
                copy.start()

    for k, copies in enumerate(moves):
        @pl.when(step == k)
        def _():
            for copy in copies:
                copy.wait()
            out_ref[ALL] = own[ALL] if k == 0 else far[k - 1].astype(BF16)


def from_slots(me, slots, num, limit):
    rows = len(slots[0])
    return call(functools.partial(from_slots_body, num), (4,), [ANYWHERE] * len(slots),
                pl.BlockSpec((rows, LANES), lambda d, me: (me[0] ^ d, 0)), sds((limit, LANES), BF16),
                slot_buffers(rows, num), prefetch=1)(me, *slots)


def unpack_body(per, half_ref, *refs):
    near, far, outs = refs[:2], refs[2:6], refs[6:]
    for k, refs_of in enumerate((near[:1] * 2, near[1:] * 2, far[:2], far[2:])):
        dst = slice(k * LANES, (k + 1) * LANES)
        for p, out in enumerate(outs):
            src = pl.ds(p % per * LANES, LANES)
            if k < 2:
                out[dst, :] = refs_of[0][p // per, src, :].astype(BF16)
                continue
            for mine in range(2):
                @pl.when(half_ref[0] == mine)
                def _():
                    out[dst, :] = refs_of[p // per ^ mine][src, :].astype(BF16)


def unpack_weights(half, slots, per):
    width = wide(slots[0])
    outs = [sds((4 * LANES, width), BF16)] * (2 * per)
    return call(functools.partial(unpack_body, per), (1,), [whole_spec(s.shape) for s in slots],
                [whole_spec(o.shape) for o in outs], outs, [], prefetch=1)(half, *slots)


IN_CUTS = (20,)
GRAD_CUTS = (4, 9, 7)
OUT_CUTS = (11, 9)


class Layer(NamedTuple):
    w1: Any
    ws: Any
    wr: Any
    w2t: Any
    vec: Any
    b1: Any
    node_w1: Any
    node_w2t: Any
    node_vec: Any
    node_b1: Any


def solution(mesh):
    lat_spec = P('dp', None, 'tp')
    first_spec = P(None, None, 'tp', None)
    col_spec = P(None, None, 'tp')
    param_specs = (first_spec, P(), col_spec, col_spec, first_spec, P(), col_spec, col_spec)
    in_specs = (lat_spec, lat_spec, P(), P(), lat_spec, lat_spec) + param_specs
    out_specs = (lat_spec, lat_spec, lat_spec, lat_spec) + param_specs
    tp = mesh.shape['tp']

    def swap(val, mask):
        return lax.ppermute(val, 'tp', [(i, i ^ mask) for i in range(tp)])

    def swap_dp(val):
        return lax.ppermute(val, 'dp', [(0, 1), (1, 0)])

    def local_step(node_lat, edge_lat, senders, receivers, grad_node, grad_edge,
                   edge_w1, edge_b1, edge_w2, edge_vec, node_w1, node_b1, node_w2, node_vec):
        me, half = lax.axis_index('tp'), lax.axis_index('dp')
        _, nodes, _ = node_lat.shape
        _, edges, _ = edge_lat.shape
        width = wide(edge_b1)
        rows = -(-edges // (tp * EDGE_BLK)) * EDGE_BLK
        pad_nodes = (nodes // NODE_BLK + 1) * NODE_BLK
        me_ref, half_ref = me.astype(jnp.int32)[None], half.astype(jnp.int32)[None]

        def to_rows(val, cuts):
            own, near, *far = to_slots(me_ref, val, rows, cuts)
            num = len(cuts)
            moved = [swap(part, 2 + k // num) for k, part in enumerate(far)]
            return [own, swap(near, 1)] + moved

        def to_columns(parts, cuts):
            own, near, *far = parts
            num = len(cuts)
            moved = [swap(part, 2 + k // num) for k, part in enumerate(far)]
            return from_slots(me_ref, [own, swap(near, 1)] + moved, num, edges)[None]

        def my_index(ids):
            padded = jnp.pad(ids, (0, tp * rows - edges), constant_values=nodes)
            return lax.dynamic_slice(padded, (me * rows,), (rows,)) * 4

        def node_slots(val):
            padded = jnp.pad(val, ((0, pad_nodes - nodes), (0, 0)))
            val = padded.astype(F32)
            far = swap(val, 2)
            return [padded, swap(val, 1), far, swap(far, 1)]

        def weight_slots(val):
            far = swap(lax.dynamic_index_in_dim(val, half, 0, keepdims=False), 2)
            rest = swap_dp(far)
            return [val, swap(val, 1), far, rest, swap(far, 1), swap(rest, 1)]

        def pack(l, w1, w2):
            return jnp.concatenate([w1[l].reshape(-1, width), w2[l].T], axis=0).astype(F32)

        vecs = jnp.concatenate([edge_vec.reshape(-1), node_vec.reshape(-1)]).reshape(-1, width)
        vecs = jnp.pad(vecs, ((0, 8 - len(vecs)), (0, 0)))
        group_a = jnp.concatenate([pack(0, edge_w1, edge_w2).reshape(2, -1, width), jnp.stack([vecs, vecs])], axis=1)
        group_b = jnp.concatenate([pack(0, node_w1, node_w2), pack(1, edge_w1, edge_w2), pack(1, node_w1, node_w2)])
        v_slots = node_slots(node_lat[0])
        slots_a = weight_slots(group_a)
        x_slots = to_rows(edge_lat[0], IN_CUTS)
        slots_b = weight_slots(group_b.reshape(2, -1, width))
        g_slots = to_rows(grad_edge[0], GRAD_CUTS)
        gn_slots = node_slots(grad_node[0])
        snd, rcv = my_index(senders), my_index(receivers)

        mats_a = unpack_weights(half_ref, slots_a, 2)
        mats_b = unpack_weights(half_ref, slots_b, 5)
        nv0, ns0, nt0, *edge_mats, nv1, ns1, nt1 = mats_b
        own_a, near_a, far_a, _, cross_a, _ = slots_a
        vec_rows = [s[2 * LANES:2 * LANES + 3].reshape(2, 2, 3, LANES) for s in (own_a[0], near_a[0], far_a, cross_a)]
        (vec0, vec1), (nvec0, nvec1) = jnp.pad(jnp.concatenate(vec_rows, axis=-1), ((0, 0), (0, 0), (0, 5), (0, 0)))
        (eb0, eb1), (nb0, nb1) = [jnp.broadcast_to(b[:, None], (2, 8, width)) for b in (edge_b1, node_b1)]
        low = Layer(*mats_a, vec0, eb0, jnp.stack([nv0, ns0]), nt0, nvec0, nb0)
        top = Layer(*edge_mats, vec1, eb1, jnp.stack([nv1, ns1]), nt1, nvec1, nb1)

        def all_sum(pair_a, pair_b):
            chip = pair_a + swap(pair_b, 1)
            total = chip + swap(chip, 2)[::-1]
            return total, swap(total, 1)

        def own_sum(pair_a, pair_b):
            chip = pair_a + swap(pair_b, 1)
            return chip[0] + swap(chip[1], 2)

        v0, ps, pr = node_project(v_slots, low.ws, low.wr, low.b1)
        hid0, nrm0, inv0, e1, sa, sb = edge_forward(
            snd, rcv, x_slots, ps, pr, low.w1, low.w2t, low.vec, (), pad_nodes)
        sa, sb = all_sum(sa, sb)
        v1, s0, nhid, nnrm, ninv, ps, pr = node_forward(
            v0, sa, sb, low.node_w1, low.node_w2t, low.node_vec, low.node_b1, top.ws, top.wr, top.b1)
        hid1, nrm1, inv1, *parts, sa, sb = edge_forward(
            snd, rcv, [e1], ps, pr, top.w1, top.w2t, top.vec, OUT_CUTS, pad_nodes)
        edge_out = to_columns(parts, OUT_CUTS)
        sa, sb = all_sum(sa, sb)

        v2, ds, dv, gn1, ndb1 = node_top(
            v1, sa, sb, gn_slots, top.node_w1, top.node_w2t, top.node_vec, top.node_b1)
        node_out = v2[:nodes][None]

        def mine_only(db1):
            lane = lax.broadcasted_iota(jnp.int32, db1.shape, 1)
            return jnp.broadcast_to(jnp.where(lane // LANES == me, db1, 0.0).sum(axis=0), db1.shape)

        d_e1, dw1e, dw2t, small, ts, tr = edge_backward(
            snd, rcv, g_slots, [e1], (hid1, nrm1, inv1), ds, top.w1, top.w2t, top.vec,
            GRAD_CUTS, pad_nodes)
        da, db, *ge1 = proj_backward(ts, tr, v1, top.ws, top.wr, dw1e, dw2t, small, mine_only(ndb1))
        da, db = all_sum(da, db)
        ds, dv_own, gn0, ndb1 = node_backward(
            dv, da, db, v0, s0, (nhid, nnrm, ninv), low.node_w1, low.node_w2t, low.node_vec)
        *d_slots, dw1e, dw2t, small, ts, tr = edge_backward(
            snd, rcv, [d_e1], x_slots, (hid0, nrm0, inv0), ds, low.w1, low.w2t, low.vec,
            (), pad_nodes)
        d_edge = to_columns(d_slots, IN_CUTS)
        da, db, *ge0 = proj_backward(ts, tr, v0, low.ws, low.wr, dw1e, dw2t, small, mine_only(ndb1))
        d_node = (dv_own + own_sum(da, db))[:nodes].astype(BF16)[None]

        def grad_sum(pair_a, pair_b):
            chip = (pair_a + swap(pair_b, 1)).reshape(2, 2, -1, width)
            keep, give = [lax.dynamic_index_in_dim(chip, h, 1, keepdims=False) for h in (half, 1 - half)]
            part = keep + swap_dp(give)
            own = part[0] + swap(part[1], 2)
            rest = swap_dp(own)
            return jnp.concatenate([jnp.where(half == h, own, rest) for h in range(2)])

        ge = [grad_sum(*ge0), grad_sum(*ge1)]
        gn = [g + swap_dp(g) for g in (gn0, gn1)]
        stack = lambda fn: jnp.stack([fn(l) for l in range(2)])
        w1_rows, w2_rows, vec_wide = 3 * LANES, 4 * LANES, 3 * LANES
        return (node_out, edge_out, d_node, d_edge,
                stack(lambda l: ge[l][:w1_rows].reshape(3, LANES, width)),
                stack(lambda l: ge[l][w2_rows + 1]),
                stack(lambda l: ge[l][w1_rows:w2_rows].T),
                stack(lambda l: ge[l][w2_rows, :vec_wide].reshape(3, LANES)),
                stack(lambda l: gn[l][:2 * LANES].reshape(2, LANES, width)),
                stack(lambda l: ge[l][w2_rows + 2]),
                stack(lambda l: gn[l][2 * LANES:w1_rows].T),
                stack(lambda l: gn[l][w1_rows:, :vec_wide].sum(axis=0).reshape(3, LANES)))

    return jax.shard_map(local_step, mesh=mesh, in_specs=in_specs, out_specs=out_specs, check_vma=False)
```
